32 devices in a mesh: frame: 8 (over y, x, core), row: 4 (over z).
Axes of the slice: x: 2, y: 2, z: 4, core: 2. Of those that a mesh axis runs over, the one named last changes fastest.
Arguments:
- tokens: bfloat16 [8, 512, 2048], P('frame', 'row'), may hold values from -6 to 6
- w_gate: bfloat16 [2048, 4096], P(None, 'row'), may hold values from -0.125 to 0.125
- w_value: bfloat16 [2048, 4096], P(None, 'row'), may hold values from -0.125 to 0.125
- w_state_proj: bfloat16 [2048, 512], replicated, may hold values from -0.03125 to 0.03125
- w_step: bfloat16 [2, 2048, 64], P(None, None, 'row'), may hold values from -0.125 to 0.125
- step_bias: float32 [2, 64], P(None, 'row'), may hold values from -3 to 0
- decay_rate: float32 [2, 64], P(None, 'row'), may hold values from 0 to 0.3, as said below
- conv_taps: float32 [2, 4, 4096], P(None, None, 'row'), may hold values from -3 to 3
- skip_gain: float32 [2, 64], P(None, 'row'), may hold values from 0.1 to 16, as said below
- norm_gain: float32 [4096], P('row'), may hold values from 0.1 to 1.9
- w_out: bfloat16 [4096, 2048], P('row'), may hold values from -0.09375 to 0.09375
Outputs:
- mixed: bfloat16 [8, 512, 2048], P('frame', 'row')
The draws below stay inside these ranges and needn't reach their ends.
Inputs may be any that keep to these rules, and one draw needn't show every extreme that they name: `decay_rate`: positive decay rates. `skip_gain`: positive skip weights.
All inputs are finite; a program needn't handle non-finite values.
Results may differ from the reference program's by a relative error of at most 0.015.
Values may be sent and summed in bfloat16 or wider, within the bound.
No kernel may reach another device: no remote copies, remote signals or barrier semaphores. Data moves between devices by JAX's collectives and lax.ppermute only.
A program may use at most 128 MiB of HBM per device.

```python
import jax
import jax.numpy as jnp
from jax import lax

D = 2048
D_INNER = 4096
HEADS = 64
HEAD_DIM = 64
STATE = 128
PATCHES = 512
CONV = 4
BLK = 128
FRAMES = 8


def draw_decay_rate(key, part):
    first, second, third = jax.random.split(jax.random.fold_in(key, 7), 3)
    share = 0.5
    quick_mask = jax.random.uniform(first, (2, HEADS)) < share
    slow_rate = jnp.exp(jax.random.uniform(second, (2, HEADS), minval=jnp.log(0.5), maxval=jnp.log(2.0))) / (0.4 * FRAMES * PATCHES)
    quick_rate = jnp.exp(jax.random.uniform(third, (2, HEADS), minval=jnp.log(0.05), maxval=jnp.log(0.3)))
    return jnp.where(quick_mask, quick_rate, slow_rate).astype(jnp.float32)


def draw_skip_gain(key, part):
    second = jax.random.fold_in(jax.random.fold_in(key, 11), 1)
    value = jnp.exp(jax.random.uniform(second, (2, HEADS), minval=jnp.log(0.25), maxval=jnp.log(8.0)))
    return value.astype(jnp.float32)


def levels(own_key, shape, pieces, least, largest):
    factor_of, own = 1.0, jax.random.fold_in(own_key, 6)
    for axis_at, parts in pieces:
        heights = jnp.exp(jax.random.uniform(jax.random.fold_in(own, axis_at), (parts,), jnp.float32, least / len(pieces), largest / len(pieces)))
        factor_of = factor_of * jnp.repeat(heights, shape[axis_at] // parts).reshape([-1 if axis == axis_at else 1 for axis in range(len(shape))])
    return factor_of


def normal_values(key, extent, scale, most, cuts=(), dtype=jnp.bfloat16):
    loudness = levels(key, extent, cuts, -0.22, 0.18) if cuts else 1.0
    values = jax.random.normal(key, extent, jnp.float32) * scale * loudness
    return jnp.minimum(jnp.maximum(values, -most), most).astype(dtype)


def setup_inputs(seed: int = 0) -> dict:
    splits = jax.random.split(jax.random.key(seed), 12)
    return {
        "tokens": normal_values(splits[0], (FRAMES, PATCHES, D), 1.0, 6.0, ((0, 8), (1, 4))),
        "w_gate": normal_values(splits[1], (D, D_INNER), D ** -0.5, 0.125, ((1, 4),)),
        "w_value": normal_values(splits[2], (D, D_INNER), D ** -0.5, 0.125, ((1, 4),)),
        "w_state_proj": normal_values(splits[3], (D, 4 * STATE), (16 * D) ** -0.5, 0.03125),
        "w_step": normal_values(splits[4], (2, D, HEADS), D ** -0.5, 0.125, ((2, 4),)),
        "step_bias": jnp.clip(-3.0 + 3.0 * jax.random.uniform(splits[5], (2, HEADS), jnp.float32) ** levels(splits[5], (2, HEADS), ((1, 4),), -0.2, 0.2), -3.0, 0.0),
        "decay_rate": draw_decay_rate(jax.random.fold_in(splits[11], 71), 0),
        "conv_taps": normal_values(splits[7], (2, CONV, D_INNER), CONV ** -0.5, 3.0, ((2, 4),), jnp.float32),
        "skip_gain": draw_skip_gain(jax.random.fold_in(splits[11], 71), 0),
        "norm_gain": jnp.clip(1.0 + 0.18 * jax.random.normal(splits[9], (D_INNER,), jnp.float32), 0.1, 1.9),
        "w_out": normal_values(splits[10], (D_INNER, D), D_INNER ** -0.5, 0.09375, ((0, 4),)),
    }


def block_weights(scores, log_cum, dt_block):
    size = scores.shape[0]
    row_index = lax.broadcasted_iota(jnp.int32, (size, size), 0)
    col_index = lax.broadcasted_iota(jnp.int32, (size, size), 1)
    causal = row_index >= col_index
    log_gap = log_cum.T[:, :, None] - log_cum.T[:, None, :]
    fading = jnp.exp(jnp.where(causal[None], log_gap, -jnp.inf))
    return (scores[None] * fading * dt_block.T[:, None, :]).astype(jnp.bfloat16)

def scan_direction(values, b_rows, c_rows, dt_rows, rate_row, skip_row):
    tok_count = values.shape[0]
    block_count = tok_count // BLK
    blocks = (values.reshape(block_count, BLK, HEADS, HEAD_DIM), b_rows.reshape(block_count, BLK, STATE), c_rows.reshape(block_count, BLK, STATE), dt_rows.reshape(block_count, BLK, HEADS))

    def advance(carry_state, block):
        x_block, b_block, c_block, dt_block = block
        log_cum = jnp.cumsum(-dt_block * rate_row[None, :], axis=0)
        scores = jnp.dot(c_block, b_block.T, preferred_element_type=jnp.float32)
        weights = block_weights(scores, log_cum, dt_block)
        x_wide = x_block.astype(jnp.float32)
        inner_out = jnp.einsum('hts,shp->thp', weights.astype(jnp.float32), x_wide)
        state_b = carry_state.astype(jnp.bfloat16)
        carried_out = jnp.einsum('tn,hpn->thp', c_block.astype(jnp.float32), state_b.astype(jnp.float32))
        result = inner_out + carried_out * jnp.exp(log_cum)[:, :, None] + skip_row[None, :, None] * x_wide
        log_last = log_cum[-1]
        carried = ((jnp.exp(log_last[None, :] - log_cum) * dt_block)[:, :, None] * x_wide).astype(jnp.bfloat16)
        update = jnp.einsum('sn,shp->hpn', b_block.astype(jnp.float32), carried.astype(jnp.float32))
        return (jnp.exp(log_last)[:, None, None] * carry_state + update, result)
    state_zero = jnp.zeros((HEADS, HEAD_DIM, STATE), jnp.float32)
    unused_state, outputs = lax.scan(advance, state_zero, blocks)
    return outputs.reshape(tok_count, HEADS, HEAD_DIM)

def conv_pass(padded, taps, tok_count, backward):
    reach = taps.shape[0] - 1
    running = jnp.zeros((tok_count, padded.shape[1]), jnp.float32)
    for tap_index in range(taps.shape[0]):
        first_row = 2 * reach - tap_index if backward else tap_index
        running = running + taps[tap_index][None, :] * padded[first_row:first_row + tok_count]
    return jax.nn.silu(running).astype(jnp.bfloat16)

def reference(tokens, w_gate, w_value, w_state_proj, w_step, step_bias, decay_rate, conv_taps, skip_gain, norm_gain, w_out):
    tok_count = FRAMES * PATCHES
    flat = tokens.reshape(tok_count, D)

    def project(matrix):
        return jnp.dot(flat, matrix, preferred_element_type=jnp.float32).astype(jnp.bfloat16)
    gate_in = project(w_gate)
    x_raw = project(w_value)
    bc_cols = project(w_state_proj)
    dt_forward = jax.nn.softplus(project(w_step[0]).astype(jnp.float32) + step_bias[0][None, :])
    dt_backward = jax.nn.softplus(project(w_step[1]).astype(jnp.float32) + step_bias[1][None, :])
    padded = jnp.pad(x_raw.astype(jnp.float32), ((CONV - 1, CONV - 1), (0, 0)))
    x_forward = conv_pass(padded, conv_taps[0], tok_count, False).reshape(tok_count, HEADS, HEAD_DIM)
    x_backward = conv_pass(padded, conv_taps[1], tok_count, True).reshape(tok_count, HEADS, HEAD_DIM)
    y_forward = scan_direction(x_forward, bc_cols[:, :STATE], bc_cols[:, STATE:2 * STATE], dt_forward, decay_rate[0], skip_gain[0])
    y_backward = jnp.flip(scan_direction(jnp.flip(x_backward, 0), jnp.flip(bc_cols[:, 2 * STATE:3 * STATE], 0), jnp.flip(bc_cols[:, 3 * STATE:], 0), jnp.flip(dt_backward, 0), decay_rate[1], skip_gain[1]), 0)
    summed = (y_forward + y_backward).reshape(tok_count, D_INNER)
    gated = summed * jax.nn.silu(gate_in.astype(jnp.float32))
    scale = lax.rsqrt(lax.optimization_barrier(jnp.mean(gated * gated, axis=-1, keepdims=True)) + 1e-05)
    normed = (gated * scale * norm_gain[None, :]).astype(jnp.bfloat16)
    mixed = jnp.dot(normed, w_out, preferred_element_type=jnp.float32).astype(jnp.bfloat16)
    return mixed.reshape(FRAMES, PATCHES, D)
```

```python
import math

import jax
import jax.numpy as jnp
from jax import lax
from jax.experimental import pallas as pl
from jax.experimental.pallas import tpu as pltpu
from jax.sharding import PartitionSpec as P

HEAD_DIM = 64
BLK = 128
LANES = 128
LOG2E = 1.0 / math.log(2.0)
F32 = jnp.float32
BF16 = jnp.bfloat16


def mib(size):
    return pltpu.CompilerParams(vmem_limit_bytes=size << 20)


def vmem():
    return pl.BlockSpec(memory_space=pltpu.VMEM)


def smem():
    return pl.BlockSpec(memory_space=pltpu.SMEM)


def dot(a, b):
    return jnp.dot(a, b, preferred_element_type=F32)


def silu(v):
    return v / (1.0 + jnp.exp(-v))


def two_parts(v, stride):
    high = v.astype(BF16).astype(F32)
    return (high + pltpu.roll(v - high, stride, 1)).astype(BF16)


def project(pieces, w_gate, w_value, w_state, w_small):
    rows, depth = sum(p.shape[0] for p in pieces), pieces[0].shape[1]
    channels, states, small = w_gate.shape[1], w_state.shape[1], w_small.shape[1]
    steps = states // LANES
    tile = channels // steps
    count = len(pieces)

    def body(*refs):
        wg, wv, ws, wt, gate, x, bc, st, stacked = refs[count:]

        @pl.when(pl.program_id(0) == 0)
        def _():
            at = 0
            for ref in refs[:count]:
                stacked[at : at + ref.shape[0], :] = ref[...]
                at += ref.shape[0]
            st[...] = dot(stacked[...], wt[...]).astype(BF16)

        lhs = stacked[...]
        x[...] = dot(lhs, wv[...]).astype(BF16)
        bc[...] = dot(lhs, ws[...]).astype(BF16)
        gate[...] = dot(lhs, wg[...]).astype(BF16)

    def col(width):
        return pl.BlockSpec((rows, width), lambda n: (0, n))

    def wcol(width):
        return pl.BlockSpec((depth, width), lambda n: (0, n))

    width = 2 * channels + states + small
    return pl.pallas_call(
        body,
        grid=(steps,),
        in_specs=[pl.BlockSpec(p.shape, lambda n: (0, 0)) for p in pieces]
        + [wcol(tile), wcol(tile), wcol(LANES), pl.BlockSpec((depth, small), lambda n: (0, 0))],
        out_specs=[col(tile), col(tile), col(LANES), pl.BlockSpec((rows, small), lambda n: (0, 0))],
        out_shape=[jax.ShapeDtypeStruct((rows, n), BF16) for n in (channels, channels, states, small)],
        scratch_shapes=[pltpu.VMEM((rows, depth), BF16)],
        compiler_params=mib(24),
        cost_estimate=pl.CostEstimate(
            flops=2 * rows * depth * width, bytes_accessed=2 * depth * width, transcendentals=0
        ),
        name="project",
    )(*pieces, w_gate, w_value, w_state, w_small)


def frame_states(where, order, rows_of, xs, before, after, bcs, sts, taps, bias, rate, spread, heads):
    channels, states = xs[0].shape[1], bcs[0].shape[1]
    size = states // 4
    ring = len(order)
    tokens = ring * rows_of
    blocks = tokens // BLK
    reach = taps.shape[0] // 2 - 1
    count = len(xs)
    pad = before.shape[0]
    groups = [[]]
    for k in order:
        if len(groups[-1]) * rows_of == xs[len(groups) - 1].shape[0]:
            groups.append([])
        groups[-1].append(k)

    def body(where, *refs):
        x_in, refs = refs[:count], refs[count:]
        bc_in, refs = refs[:count], refs[count:]
        st_in, refs = refs[:count], refs[count:]
        before, after, taps, bias, rate, spread = refs[:6]
        xf, xb, bc, cum_out, cum_t, etot, starts, pack = refs[6:14]
        sx, raw, qs, bt = refs[14:]
        mine = where[0]
        sx[0:pad, :] = before[...].astype(F32)
        sx[pad + tokens :, :] = after[...].astype(F32)
        for refx, refb, refs_, ks in zip(x_in, bc_in, st_in, groups):
            for i, k in enumerate(ks):
                row = pl.multiple_of(lax.rem(mine + k, ring) * rows_of, rows_of)
                part = slice(i * rows_of, (i + 1) * rows_of)
                sx[pl.ds(row + pad, rows_of), :] = refx[part, :].astype(F32)
                bc[pl.ds(row, rows_of), :] = refb[part, :]
                raw[pl.ds(row, rows_of), :] = refs_[part, :].astype(F32)

        def conv(i, carry):
            cols = pl.ds(pl.multiple_of(i * LANES, LANES), LANES)
            tap = taps[:, cols]
            for base in range(0, tokens, 64):
                views = {
                    o: sx[base + pad + o : base + pad + o + 64, cols] for o in range(-reach, reach + 1)
                }
                f = sum(tap[j : j + 1] * views[j - reach] for j in range(reach + 1))
                b = sum(tap[reach + 1 + j : reach + 2 + j] * views[reach - j] for j in range(reach + 1))
                xf[base : base + 64, cols] = silu(f).astype(BF16)
                xb[base : base + 64, cols] = silu(b).astype(BF16)
            return carry

        lax.fori_loop(0, channels // LANES, conv, 0)

        lane = lax.broadcasted_iota(jnp.int32, (BLK, LANES), 1)
        used = lane < 2 * heads
        forward = lane < heads
        low_row, low_col = (lax.broadcasted_iota(jnp.int32, (BLK, BLK), d) for d in (0, 1))
        both = jnp.concatenate(
            [
                jnp.where(low_row >= low_col, 1.0, 0.0).astype(BF16),
                jnp.where(low_row <= low_col, 1.0, 0.0).astype(BF16),
            ],
            axis=0,
        )
        cums, dts, lasts = [], [], []
        for b in range(blocks):
            rows = slice(b * BLK, (b + 1) * BLK)
            v = raw[rows, :] + bias[...]
            dt = jnp.maximum(v, 0.0) + jnp.log1p(jnp.exp(-jnp.abs(v)))
            dt = jnp.where(used, dt, 0.0)
            a = -dt * rate[...] * LOG2E
            a1 = a.astype(BF16).astype(F32)
            a2 = (a - a1).astype(BF16).astype(F32)
            a3 = a - a1 - a2
            parts = a1 + pltpu.roll(a2, 2 * heads, 1) + pltpu.roll(a3, 4 * heads, 1)
            sums = dot(both, parts.astype(BF16))
            sums = (
                pltpu.roll(sums, LANES - 4 * heads, 1) + pltpu.roll(sums, LANES - 2 * heads, 1) + sums
            )
            cum = jnp.where(used, jnp.where(forward, sums[:BLK], sums[BLK:]), 0.0)
            last = jnp.where(forward[:1], cum[BLK - 1 :], cum[:1])
            cum_out[rows, :] = cum
            cum_t[rows, :] = (cum + pltpu.roll(dt, 2 * heads, 1)).T
            q = jnp.exp2(last - cum) * dt
            qs[rows, :] = two_parts(q, 2 * heads)
            cums.append(cum)
            lasts.append(last)
        total = sum(lasts[1:], lasts[0])
        off_f = jnp.zeros_like(total)
        off_b = total
        decay_rows = []
        for b in range(blocks):
            off_b = off_b - lasts[b] if b < blocks - 1 else jnp.zeros_like(total)
            off = jnp.where(forward[:1], off_f, off_b)
            e = jnp.where(used, jnp.exp2(cums[b] + off), 0.0)
            etot[b * BLK : (b + 1) * BLK, :] = two_parts(e, 2 * heads)
            off_f = off_f + lasts[b]
            decay_rows.append(jnp.where(used[:1], jnp.exp2(lasts[b]), 0.0))
        fill = jnp.zeros((8 - blocks % 8, LANES), F32) if blocks % 8 else None
        decays = jnp.concatenate(decay_rows + ([fill] if fill is not None else []), axis=0)
        l1 = total.astype(BF16).astype(F32)
        l2 = (total - l1).astype(BF16).astype(F32)
        l3 = total - l1 - l2
        logs = jnp.concatenate([l1, l2, l3, jnp.zeros((13, LANES), F32)], axis=0).astype(BF16)
        decays = two_parts(decays, 2 * heads)
        for d in range(2):
            at = d * 2 * size
            for b in range(blocks):
                bt[b] = bc[b * BLK : (b + 1) * BLK, at : at + size].astype(F32).T.astype(BF16)
            x_dir = (xf, xb)[d]
            for c in range(0, channels, 256):
                cols = slice(c, c + 256)
                fade = dot(decays, spread[d, :, cols])
                state = jnp.zeros((size, 256), F32)
                for b in range(blocks) if d == 0 else range(blocks - 1, -1, -1):
                    rows = slice(b * BLK, (b + 1) * BLK)
                    starts[d, b, :, cols] = state.astype(BF16)
                    scale = dot(qs[rows, :], spread[d, :, cols])
                    carried = (scale * x_dir[rows, cols].astype(F32)).astype(BF16)
                    state = fade[b : b + 1] * state + dot(bt[b], carried)
                pack[d, 0:size, cols] = state.astype(BF16)
                pack[d, size:, cols] = dot(logs, spread[d, :, cols]).astype(BF16)

    shapes = [
        ((tokens, channels), BF16),
        ((tokens, channels), BF16),
        ((tokens, states), BF16),
        ((tokens, LANES), F32),
        ((tokens, LANES), F32),
        ((tokens, LANES), BF16),
        ((2, blocks, size, channels), BF16),
        ((2, size + 16, channels), BF16),
    ]
    return pl.pallas_call(
        body,
        in_specs=[smem()] + [vmem()] * (3 * count + 6),
        out_specs=[vmem()] * len(shapes),
        out_shape=[jax.ShapeDtypeStruct(*s) for s in shapes],
        scratch_shapes=[
            pltpu.VMEM((tokens + 2 * pad, channels), F32),
            pltpu.VMEM((tokens, LANES), F32),
            pltpu.VMEM((tokens, LANES), BF16),
            pltpu.VMEM((blocks, size, BLK), BF16),
        ],
        compiler_params=mib(32),
        cost_estimate=pl.CostEstimate(flops=4_000_000_000, bytes_accessed=6 << 20, transcendentals=0),
        name="frame_states",
    )(where, *xs, *bcs, *sts, before, after, taps, bias, rate, spread)


def inside(xf, xb, bc, cum, cum_t, starts, skip, heads):
    tokens, channels = xf.shape
    states = bc.shape[1]
    size = states // 4
    blocks = tokens // BLK

    def body(xf, xb, bc, cum, cum_t, starts, skip, y):
        row, col = (lax.broadcasted_iota(jnp.int32, (BLK, BLK), d) for d in (0, 1))
        first = lax.broadcasted_iota(jnp.int32, (BLK, LANES), 1) < HEAD_DIM
        xs = (xf, xb)
        scores, outs = [], []
        for d in range(2):
            b_rows = bc[:, 2 * d * size : (2 * d + 1) * size]
            c_rows = bc[:, (2 * d + 1) * size : (2 * d + 2) * size]
            s = lax.dot_general(c_rows, b_rows, (((1,), (1,)), ((), ())), preferred_element_type=F32)
            scores.append(jnp.where(row >= col if d == 0 else row <= col, s, 0.0))
            outs.append(c_rows)
        for pair in range(channels // LANES):
            cols = slice(pair * LANES, (pair + 1) * LANES)
            weights = []
            reached = [[], []]
            for i in range(2):
                h = 2 * pair + i
                sides = []
                for d in range(2):
                    at = d * heads + h
                    mine = jnp.broadcast_to(cum[:, at : at + 1], (BLK, BLK))
                    gap = jnp.minimum(mine - cum_t[at : at + 1, :], 0.0)
                    dt = cum_t[2 * heads + at : 2 * heads + at + 1, :]
                    sides.append((jnp.exp2(gap) * (scores[d] * dt)).astype(BF16))
                    reached[d].append(mine)
                weights.append(jnp.concatenate(sides, axis=1))
            x_pair = jnp.concatenate([xf[:, cols], xb[:, cols]], axis=0)
            out = dot(jnp.concatenate(weights, axis=0), x_pair)
            total = jnp.where(first, out[:BLK], out[BLK:])
            for d in range(2):
                fade = jnp.exp2(jnp.where(first, reached[d][0], reached[d][1]))
                total += fade * dot(outs[d], starts[d, 0, :, cols])
                total += skip[d : d + 1, cols] * xs[d][:, cols].astype(F32)
            y[:, cols] = total

    def rows(width):
        return pl.BlockSpec((BLK, width), lambda b: (b, 0))

    return pl.pallas_call(
        body,
        grid=(blocks,),
        in_specs=[
            rows(channels),
            rows(channels),
            rows(states),
            rows(LANES),
            rows(LANES),
            pl.BlockSpec((2, 1, size, channels), lambda b: (0, b, 0, 0)),
            pl.BlockSpec(skip.shape, lambda b: (0, 0)),
        ],
        out_specs=rows(channels),
        out_shape=jax.ShapeDtypeStruct((tokens, channels), F32),
        compiler_params=mib(24),
        cost_estimate=pl.CostEstimate(flops=6_000_000_000, bytes_accessed=6 << 20, transcendentals=0),
        name="inside",
    )(xf, xb, bc, cum, cum_t, starts, skip)


def logs_of(ref, lead, size):
    rows = ref[lead + (slice(size, size + 16), slice(None))].astype(F32)
    return rows[0:1] + rows[1:2] + rows[2:3]


def messages(where, mine, theirs, groups):
    size, channels = mine.shape[1] - 16, mine.shape[2]

    def body(where, mine, theirs, *outs):
        group, second = where[1], where[2] == 1
        for d in range(2):
            own, other = logs_of(mine, (d,), size), logs_of(theirs, (d,), size)
            later = second if d == 0 else jnp.logical_not(second)
            scale_own = jnp.where(later, 1.0, jnp.exp2(other))
            scale_other = jnp.where(later, jnp.exp2(own), 1.0)
            total = own + other
            l1 = total.astype(BF16).astype(F32)
            l2 = (total - l1).astype(BF16).astype(F32)
            logs = jnp.concatenate([l1, l2, total - l1 - l2, jnp.zeros((13, channels), F32)], axis=0)
            state = scale_own * mine[d, :size, :].astype(F32) + scale_other * theirs[d, :size, :].astype(F32)
            state = state.astype(BF16)
            for k, out in enumerate(outs, 1):
                onward = group + k < groups

                @pl.when(onward if d == 0 else jnp.logical_not(onward))
                def _(out=out):
                    out[:size, :] = state
                    out[size:, :] = logs.astype(BF16)

    return pl.pallas_call(
        body,
        in_specs=[smem(), vmem(), vmem()],
        out_specs=[vmem()] * (groups - 1),
        out_shape=[jax.ShapeDtypeStruct(mine.shape[1:], BF16)] * (groups - 1),
        compiler_params=mib(16),
        cost_estimate=pl.CostEstimate(flops=1_000_000, bytes_accessed=2 << 20, transcendentals=0),
        name="messages",
    )(where, mine, theirs)


def entering(where, theirs, received, groups):
    size, channels = theirs.shape[1] - 16, theirs.shape[2]

    def body(where, theirs, *refs):
        got, out = refs[:-1], refs[-1]
        group, second = where[1], where[2] == 1
        for d in range(2):
            near = second if d == 0 else jnp.logical_not(second)
            log = jnp.where(near, logs_of(theirs, (d,), size), 0.0)
            state = jnp.where(near, 1.0, 0.0) * theirs[d, :size, :].astype(F32)
            for far in range(1, groups):
                ref = got[far - 1] if d == 0 else got[groups - far - 1]
                holds = far <= (group if d == 0 else groups - 1 - group)
                scale = jnp.where(holds, jnp.exp2(log), 0.0)
                state += scale * ref[:size, :].astype(F32)
                log = jnp.where(holds, log + logs_of(ref, (), size), log)
            out[d] = state.astype(BF16)

    return pl.pallas_call(
        body,
        in_specs=[smem()] + [vmem()] * (1 + len(received)),
        out_specs=vmem(),
        out_shape=jax.ShapeDtypeStruct((2, size, channels), BF16),
        compiler_params=mib(16),
        cost_estimate=pl.CostEstimate(flops=1_000_000, bytes_accessed=2 << 20, transcendentals=0),
        name="entering",
    )(where, theirs, *received)


def finish(where, k, ring, y, bc, etot, gate, part, enter, spread, gain, w_out, dtype):
    tokens, channels = y.shape
    rows = tokens // ring
    states = bc.shape[1]
    size = states // 4
    width = w_out.shape[1]

    def body(where, y, bc, etot, gate, enter, spread, gain, w_out, out, squares, scaled):
        square = jnp.zeros((rows, LANES), F32)
        for c in range(0, channels, 256):
            cols = slice(c, c + 256)
            total = y[:, cols]
            for d in range(2):
                c_rows = bc[:, (2 * d + 1) * size : (2 * d + 2) * size]
                total += dot(etot[...], spread[d, :, cols]) * dot(c_rows, enter[d, :, cols])
            gated = total * silu(gate[:, cols].astype(F32))
            for t in range(0, 256, LANES):
                square += gated[:, t : t + LANES] * gated[:, t : t + LANES]
            scaled[:, cols] = (gated * gain[:, cols]).astype(BF16)
        squares[...] = square
        for c in range(0, width, 512):
            out[:, c : c + 512] = dot(scaled[...], w_out[:, c : c + 512]).astype(dtype)

    def block(width):
        return pl.BlockSpec((rows, width), lambda i, w: (lax.rem(w[0] + k, ring), 0))

    def whole(shape):
        return pl.BlockSpec(shape, lambda i, w: (0,) * len(shape))

    return pl.pallas_call(
        body,
        grid_spec=pltpu.PrefetchScalarGridSpec(
            num_scalar_prefetch=1,
            grid=(1,),
            in_specs=[
                block(channels),
                block(states),
                block(LANES),
                pl.BlockSpec((rows, channels), lambda i, w: (part, 0)),
                whole(enter.shape),
                whole(spread.shape),
                whole(gain.shape),
                whole(w_out.shape),
            ],
            out_specs=[whole((rows, width)), whole((rows, LANES))],
            scratch_shapes=[pltpu.VMEM((rows, channels), BF16)],
        ),
        out_shape=[
            jax.ShapeDtypeStruct((rows, width), dtype),
            jax.ShapeDtypeStruct((rows, LANES), F32),
        ],
        compiler_params=mib(24),
        cost_estimate=pl.CostEstimate(
            flops=2 * rows * channels * width, bytes_accessed=2 * channels * width, transcendentals=0
        ),
        name="finish",
    )(where, y, bc, etot, gate, enter, spread, gain, w_out)


def ring_pairs(count, step):
    return [(i, (i + step) % count) for i in range(count)]


def per_device(
    tokens,
    w_gate,
    w_value,
    w_state_proj,
    w_step,
    step_bias,
    decay_rate,
    conv_taps,
    skip_gain,
    norm_gain,
    w_out,
):
    ring, frames = lax.axis_size("row"), lax.axis_size("frame")
    row, frame = lax.axis_index("row"), lax.axis_index("frame")
    channels, heads = w_gate.shape[1], step_bias.shape[1]
    span = 2 if frames % 2 == 0 else 1
    groups = frames // span
    where = jnp.stack([row, frame // span, frame % span]).astype(jnp.int32)
    own = tokens.reshape(-1, tokens.shape[2])
    rows = own.shape[0]
    half = rows // 2
    far = ring // 2

    def up(v):
        return lax.ppermute(v, "row", ring_pairs(ring, 1))

    def down(v):
        return lax.ppermute(v, "row", ring_pairs(ring, -1))

    arrived = []
    from_below, from_above = [own[:half], own[half:]], [own[half:], own[:half]]
    for hop in range(1, far + 1):
        ends = 2 * hop == ring
        a = up(from_below[0])
        c = down(from_above[0])
        if ends:
            arrived.append([a, c])
        else:
            b, d = up(from_below[1]), down(from_above[1])
            from_below, from_above = [a, b], [c, d]
            arrived.append([a, b, d, c])

    pad_lanes = LANES - 2 * heads
    w_small = jnp.concatenate(
        [w_step[0], w_step[1], jnp.zeros((w_step.shape[1], pad_lanes), w_step.dtype)], axis=1
    )
    bias = jnp.pad(step_bias.reshape(1, -1), ((0, 0), (0, pad_lanes)))
    rate = jnp.pad(decay_rate.reshape(1, -1), ((0, 0), (0, pad_lanes)))
    skip = jnp.repeat(skip_gain, HEAD_DIM, axis=1)
    taps = conv_taps.reshape(-1, channels)
    gain = norm_gain.reshape(1, -1)
    lane = lax.broadcasted_iota(jnp.int32, (LANES, channels), 0)
    head = lax.broadcasted_iota(jnp.int32, (LANES, channels), 1) // HEAD_DIM
    spread = jnp.stack(
        [
            ((lane == head + d * heads) | (lane == head + (2 + d) * heads)).astype(BF16)
            for d in range(2)
        ]
    )

    order, projected = [0], [project([own], w_gate, w_value, w_state_proj, w_small)]
    for hop, pieces in enumerate(arrived, 1):
        order += [ring - hop, hop] if len(pieces) == 4 else [hop]
        projected.append(project(pieces, w_gate, w_value, w_state_proj, w_small))
    gates, xs, bcs, sts = zip(*projected)
    place = {}
    at = 0
    for j, x in enumerate(xs):
        for i in range(x.shape[0] // rows):
            place[order[at]] = (j, i)
            at += 1

    edge = 8

    def pick(k, first):
        j, i = place[k]
        start = i * rows if first else (i + 1) * rows - edge
        return xs[j][start : start + edge]

    tails = jnp.stack([pick(k, False) for k in range(ring)])
    heads_of = jnp.stack([pick(k, True) for k in range(ring)])
    tail = lax.dynamic_index_in_dim(tails, (2 * ring - 1 - row) % ring, keepdims=False)
    top = lax.dynamic_index_in_dim(heads_of, (ring - row) % ring, keepdims=False)
    before = lax.ppermute(tail, "frame", [(i, i + 1) for i in range(frames - 1)])
    after = lax.ppermute(top, "frame", [(i + 1, i) for i in range(frames - 1)])

    xf, xb, bc, cum, cum_t, etot, starts, pack = frame_states(
        where, order, rows, xs, before, after, bcs, sts, taps, bias, rate, spread, heads
    )

    if span == 2:
        theirs = lax.ppermute(pack, "frame", [(i, i ^ 1) for i in range(frames)])
    else:
        theirs = jnp.zeros_like(pack)
    received = []
    if groups > 1:
        sends = messages(where, pack, theirs, groups)
        for k, send in enumerate(sends, 1):
            pairs = [
                (g * span + s, (g + k) % groups * span + s) for g in range(groups) for s in range(span)
            ]
            received.append(lax.ppermute(send, "frame", pairs))
    y = inside(xf, xb, bc, cum, cum_t, starts, skip, heads)
    enter = entering(where, theirs, received, groups)

    def block(k, dtype=BF16):
        j, i = place[k]
        value, squares = finish(
            where, k, ring, y, bc, etot, gates[j], i, enter, spread, gain, w_out, dtype
        )
        return value, jnp.sum(squares, axis=1)

    squares = []
    up_a = up_b = down_a = down_b = None
    for hop in range(far, 0, -1):
        if 2 * hop == ring:
            value, square = block(hop)
            up_a, down_b = up(value[:half]), down(value[half:])
            squares.append((hop, square))
            continue
        above, square_above = block(hop)
        below, square_below = block(ring - hop)
        squares += [(hop, square_above), (ring - hop, square_below)]

        def plus(v, w):
            return v if w is None else (v.astype(F32) + w.astype(F32)).astype(BF16)

        up_b = up(plus(above[half:], up_b))
        down_a = down(plus(below[:half], down_a))
        up_a = up(plus(above[:half], up_a))
        down_b = down(plus(below[half:], down_b))
    value, square = block(0, F32)
    for k, part in squares:
        square = square + lax.ppermute(part, "row", ring_pairs(ring, k))
    total = jnp.concatenate(
        [
            value[:half] + up_a.astype(F32) + down_a.astype(F32),
            value[half:] + up_b.astype(F32) + down_b.astype(F32),
        ],
        axis=0,
    )
    scale = lax.rsqrt(square / (channels * ring) + 1e-05)
    return (total * scale[:, None]).astype(BF16).reshape(tokens.shape)


def solution(mesh):
    return jax.shard_map(
        per_device,
        mesh=mesh,
        in_specs=(
            P("frame", "row", None),
            P(None, "row"),
            P(None, "row"),
            P(),
            P(None, None, "row"),
            P(None, "row"),
            P(None, "row"),
            P(None, None, "row"),
            P(None, "row"),
            P("row"),
            P("row", None),
        ),
        out_specs=P("frame", "row", None),
        check_vma=False,
    )
```

```python
import math

import jax
import jax.numpy as jnp
from jax import lax
from jax.experimental import pallas as pl
from jax.experimental.pallas import tpu as pltpu
from jax.sharding import PartitionSpec as P

HEAD_DIM = 64
BLK = 128
LANES = 128
LOG2E = 1.0 / math.log(2.0)
F32 = jnp.float32
BF16 = jnp.bfloat16


def mib(size):
    return pltpu.CompilerParams(vmem_limit_bytes=size << 20)


def vmem():
    return pl.BlockSpec(memory_space=pltpu.VMEM)


def smem():
    return pl.BlockSpec(memory_space=pltpu.SMEM)


def dot(a, b):
    return jnp.dot(a, b, preferred_element_type=F32)


def silu(v):
    return v / (1.0 + jnp.exp(-v))


def two_parts(v, stride):
    high = v.astype(BF16).astype(F32)
    return (high + pltpu.roll(v - high, stride, 1)).astype(BF16)


def split(where, own, ring, edge):
    rows, depth = own.shape
    half = rows // 2

    def body(where, own, a, b, ends):
        a[...] = own[:half, :]
        b[...] = own[half:, :]

        @pl.when(where[0] == ring - 1)
        def _():
            ends[...] = own[rows - edge :, :]

        @pl.when(where[0] != ring - 1)
        def _():
            ends[...] = own[:edge, :]

    shapes = [(half, depth), (half, depth), (edge, depth)]
    return pl.pallas_call(
        body,
        in_specs=[smem(), vmem()],
        out_specs=[vmem()] * 3,
        out_shape=[jax.ShapeDtypeStruct(s, BF16) for s in shapes],
        compiler_params=mib(8),
        name="split",
    )(where, own)


def prepare(step_bias, decay_rate, skip_gain, channels):
    heads = step_bias.shape[1]
    rest = LANES - 2 * heads

    def body(bias, rate, skip, spread, rows, skips):
        lane = lax.broadcasted_iota(jnp.int32, (LANES, channels), 0)
        head = lax.shift_right_logical(
            lax.broadcasted_iota(jnp.int32, (LANES, channels), 1), HEAD_DIM.bit_length() - 1
        )
        for d in range(2):
            hit = (lane == head + d * heads) | (lane == head + (2 + d) * heads)
            spread[d] = jnp.where(hit, 1.0, 0.0).astype(BF16)
        zeros = jnp.zeros((1, rest), F32)
        for at, ref in enumerate((bias, rate)):
            rows[at : at + 1, :] = jnp.concatenate([ref[0:1, :], ref[1:2, :], zeros], axis=1)
        pieces = jnp.concatenate([skip[...], jnp.zeros((2, LANES - heads), F32)], axis=1)
        p1 = pieces.astype(BF16).astype(F32)
        p2 = (pieces - p1).astype(BF16).astype(F32)
        p3 = pieces - p1 - p2
        stack = jnp.concatenate([p1, p2, p3, jnp.zeros((10, LANES), F32)], axis=0).astype(BF16)
        wide = dot(stack, spread[0])
        skips[...] = wide[0:2] + wide[2:4] + wide[4:6]

    shapes = [((2, LANES, channels), BF16), ((2, LANES), F32), ((2, channels), F32)]
    return pl.pallas_call(
        body,
        in_specs=[vmem()] * 3,
        out_specs=[vmem()] * 3,
        out_shape=[jax.ShapeDtypeStruct(*s) for s in shapes],
        compiler_params=mib(8),
        name="prepare",
    )(step_bias, decay_rate, skip_gain)


def stack_of(pieces):
    return pltpu.VMEM((sum(p.shape[0] for p in pieces), pieces[0].shape[1]), BF16)


def gather(refs, stacked):
    at = 0
    for ref in refs:
        stacked[at : at + ref.shape[0], :] = ref[...]
        at += ref.shape[0]


def project(where, pieces, bounds, w_value, w_state, w_step):
    ring = len(bounds)
    edge = bounds[0].shape[0] if bounds else 0
    rows, depth = sum(p.shape[0] for p in pieces), pieces[0].shape[1]
    total = rows + 2 * edge
    channels, states, small = w_value.shape[1], w_state.shape[1], w_step.shape[0]
    count = len(pieces)

    def body(where, *refs):
        wv, ws, wt, x, bc, st, stacked = refs[count + ring :]
        gather(refs[:count], stacked)
        for j, ref in enumerate(refs[count : count + ring]):
            @pl.when(lax.rem(where[0] + 1, ring) == j)
            def _(ref=ref):
                stacked[rows : rows + edge, :] = ref[...]

            @pl.when(where[0] == j)
            def _(ref=ref):
                stacked[rows + edge :, :] = ref[...]

        tile = 256
        for n in range(0, channels, tile):
            x[:, n : n + tile] = dot(stacked[...], wv[:, n : n + tile]).astype(BF16)
        for n in range(0, states, tile):
            bc[:, n : n + tile] = dot(stacked[:rows, :], ws[:, n : n + tile]).astype(BF16)
        st[...] = lax.dot_general(
            stacked[:rows, :], wt[...], (((1,), (1,)), ((), ())), preferred_element_type=F32
        ).astype(BF16)

    width = channels + states + LANES
    return pl.pallas_call(
        body,
        in_specs=[smem()] + [vmem()] * (count + ring + 3),
        out_specs=[vmem()] * 3,
        out_shape=[
            jax.ShapeDtypeStruct((total, channels), BF16),
            jax.ShapeDtypeStruct((rows, states), BF16),
            jax.ShapeDtypeStruct((rows, small), BF16),
        ],
        scratch_shapes=[pltpu.VMEM((total, depth), BF16)],
        compiler_params=mib(16),
        cost_estimate=pl.CostEstimate(
            flops=2 * total * depth * width, bytes_accessed=2 * depth * width, transcendentals=0
        ),
        name="project",
    )(where, *pieces, *bounds, w_value, w_state, w_step)


def gates(pieces, w_gate):
    rows, depth = sum(p.shape[0] for p in pieces), pieces[0].shape[1]
    channels = w_gate.shape[1]
    count = len(pieces)

    def body(*refs):
        wg, gate, stacked = refs[count:]
        gather(refs[:count], stacked)
        for n in range(0, channels, 256):
            raw = dot(stacked[...], wg[:, n : n + 256]).astype(BF16)
            gate[:, n : n + 256] = silu(raw.astype(F32))

    return pl.pallas_call(
        body,
        in_specs=[vmem()] * (count + 1),
        out_specs=vmem(),
        out_shape=jax.ShapeDtypeStruct((rows, channels), F32),
        scratch_shapes=[stack_of(pieces)],
        compiler_params=mib(16),
        cost_estimate=pl.CostEstimate(
            flops=2 * rows * depth * channels, bytes_accessed=2 * depth * channels, transcendentals=0
        ),
        name="gates",
    )(*pieces, w_gate)


def frame_states(where, order, rows_of, edge, xs, bcs, sts, taps, rows, spread, heads):
    channels, states = xs[0].shape[1], bcs[0].shape[1]
    size = states // 4
    ring = len(order)
    tokens = ring * rows_of
    blocks = tokens // BLK
    reach = taps.shape[1] - 1
    count = len(xs)
    pad = edge
    groups = [[]]
    for k in order:
        if len(groups[-1]) * rows_of == bcs[len(groups) - 1].shape[0]:
            groups.append([])
        groups[-1].append(k)

    def body(where, *refs):
        x_in, refs = refs[:count], refs[count:]
        bc_in, refs = refs[:count], refs[count:]
        st_in, refs = refs[:count], refs[count:]
        taps, small, spread = refs[:3]
        xf, xb, bc, cum_out, cum_t, etot, starts, pack = refs[3:11]
        sx, raw, qs, bt = refs[11:]
        mine = where[0]
        bias, rate = small[0:1, :], small[1:2, :]
        sx[0:pad, :] = x_in[0][rows_of : rows_of + pad, :].astype(F32)
        sx[pad + tokens :, :] = x_in[0][rows_of + pad :, :].astype(F32)
        raw[...] = jnp.zeros_like(raw)
        for refx, refb, refs_, ks in zip(x_in, bc_in, st_in, groups):
            for i, k in enumerate(ks):
                row = pl.multiple_of(lax.rem(mine + k, ring) * rows_of, rows_of)
                part = slice(i * rows_of, (i + 1) * rows_of)
                sx[pl.ds(row + pad, rows_of), :] = refx[part, :].astype(F32)
                bc[pl.ds(row, rows_of), :] = refb[part, :]
                raw[pl.ds(row, rows_of), 0 : 2 * heads] = refs_[part, :].astype(F32)

        def conv(i, carry):
            cols = pl.ds(pl.multiple_of(i * LANES, LANES), LANES)
            ahead, behind = taps[0, :, cols], taps[1, :, cols]
            for base in range(0, tokens, 64):
                views = {
                    o: sx[base + pad + o : base + pad + o + 64, cols] for o in range(-reach, reach + 1)
                }
                f = sum(ahead[j : j + 1] * views[j - reach] for j in range(reach + 1))
                b = sum(behind[j : j + 1] * views[reach - j] for j in range(reach + 1))
                xf[base : base + 64, cols] = silu(f).astype(BF16)
                xb[base : base + 64, cols] = silu(b).astype(BF16)
            return carry

        lax.fori_loop(0, channels // LANES, conv, 0)

        lane = lax.broadcasted_iota(jnp.int32, (BLK, LANES), 1)
        used = lane < 2 * heads
        forward = lane < heads
        low_row, low_col = (lax.broadcasted_iota(jnp.int32, (BLK, BLK), d) for d in (0, 1))
        both = jnp.concatenate(
            [
                jnp.where(low_row >= low_col, 1.0, 0.0).astype(BF16),
                jnp.where(low_row <= low_col, 1.0, 0.0).astype(BF16),
            ],
            axis=0,
        )
        cums, dts, lasts = [], [], []
        for b in range(blocks):
            rows = slice(b * BLK, (b + 1) * BLK)
            v = raw[rows, :] + bias
            dt = jnp.maximum(v, 0.0) + jnp.log1p(jnp.exp(-jnp.abs(v)))
            dt = jnp.where(used, dt, 0.0)
            a = -dt * rate * LOG2E
            a1 = a.astype(BF16).astype(F32)
            a2 = (a - a1).astype(BF16).astype(F32)
            a3 = a - a1 - a2
            parts = a1 + pltpu.roll(a2, 2 * heads, 1) + pltpu.roll(a3, 4 * heads, 1)
            sums = dot(both, parts.astype(BF16))
            sums = (
                pltpu.roll(sums, LANES - 4 * heads, 1) + pltpu.roll(sums, LANES - 2 * heads, 1) + sums
            )
            cum = jnp.where(used, jnp.where(forward, sums[:BLK], sums[BLK:]), 0.0)
            last = jnp.where(forward[:1], cum[BLK - 1 :], cum[:1])
            cum_out[rows, :] = cum
            cum_t[rows, :] = (cum + pltpu.roll(dt, 2 * heads, 1)).T
            q = jnp.exp2(last - cum) * dt
            qs[rows, :] = two_parts(q, 2 * heads)
            cums.append(cum)
            lasts.append(last)
        total = sum(lasts[1:], lasts[0])
        off_f = jnp.zeros_like(total)
        off_b = total
        decay_rows = []
        for b in range(blocks):
            off_b = off_b - lasts[b] if b < blocks - 1 else jnp.zeros_like(total)
            off = jnp.where(forward[:1], off_f, off_b)
            e = jnp.where(used, jnp.exp2(cums[b] + off), 0.0)
            etot[b * BLK : (b + 1) * BLK, :] = two_parts(e, 2 * heads)
            off_f = off_f + lasts[b]
            decay_rows.append(jnp.where(used[:1], jnp.exp2(lasts[b]), 0.0))
        fill = jnp.zeros((8 - blocks % 8, LANES), F32) if blocks % 8 else None
        decays = jnp.concatenate(decay_rows + ([fill] if fill is not None else []), axis=0)
        l1 = total.astype(BF16).astype(F32)
        l2 = (total - l1).astype(BF16).astype(F32)
        l3 = total - l1 - l2
        logs = jnp.concatenate([l1, l2, l3, jnp.zeros((13, LANES), F32)], axis=0).astype(BF16)
        decays = two_parts(decays, 2 * heads)
        for d in range(2):
            at = d * 2 * size
            for b in range(blocks):
                bt[b] = bc[b * BLK : (b + 1) * BLK, at : at + size].astype(F32).T.astype(BF16)
            x_dir = (xf, xb)[d]
            for c in range(0, channels, 256):
                cols = slice(c, c + 256)
                fade = dot(decays, spread[d, :, cols])
                state = jnp.zeros((size, 256), F32)
                for b in range(blocks) if d == 0 else range(blocks - 1, -1, -1):
                    rows = slice(b * BLK, (b + 1) * BLK)
                    starts[d, b, :, cols] = state.astype(BF16)
                    scale = dot(qs[rows, :], spread[d, :, cols])
                    carried = (scale * x_dir[rows, cols].astype(F32)).astype(BF16)
                    state = fade[b : b + 1] * state + dot(bt[b], carried)
                pack[d, 0:size, cols] = state.astype(BF16)
                pack[d, size:, cols] = dot(logs, spread[d, :, cols]).astype(BF16)

    shapes = [
        ((tokens, channels), BF16),
        ((tokens, channels), BF16),
        ((tokens, states), BF16),
        ((tokens, LANES), F32),
        ((tokens, LANES), F32),
        ((tokens, LANES), BF16),
        ((2, blocks, size, channels), BF16),
        ((2, size + 16, channels), BF16),
    ]
    return pl.pallas_call(
        body,
        in_specs=[smem()] + [vmem()] * (3 * count + 3),
        out_specs=[vmem()] * len(shapes),
        out_shape=[jax.ShapeDtypeStruct(*s) for s in shapes],
        scratch_shapes=[
            pltpu.VMEM((tokens + 2 * pad, channels), F32),
            pltpu.VMEM((tokens, LANES), F32),
            pltpu.VMEM((tokens, LANES), BF16),
            pltpu.VMEM((blocks, size, BLK), BF16),
        ],
        compiler_params=mib(20),
        cost_estimate=pl.CostEstimate(flops=4_000_000_000, bytes_accessed=6 << 20, transcendentals=0),
        name="frame_states",
    )(where, *xs, *bcs, *sts, taps, rows, spread)


def inside(xf, xb, bc, cum, cum_t, starts, skip, heads):
    tokens, channels = xf.shape
    states = bc.shape[1]
    size = states // 4
    blocks = tokens // BLK

    def body(xf, xb, bc, cum, cum_t, starts, skip, y):
        row, col = (lax.broadcasted_iota(jnp.int32, (BLK, BLK), d) for d in (0, 1))
        first = lax.broadcasted_iota(jnp.int32, (BLK, LANES), 1) < HEAD_DIM
        xs = (xf, xb)
        scores, outs = [], []
        for d in range(2):
            b_rows = bc[:, 2 * d * size : (2 * d + 1) * size]
            c_rows = bc[:, (2 * d + 1) * size : (2 * d + 2) * size]
            s = lax.dot_general(c_rows, b_rows, (((1,), (1,)), ((), ())), preferred_element_type=F32)
            scores.append(jnp.where(row >= col if d == 0 else row <= col, s, 0.0))
            outs.append(c_rows)
        for pair in range(channels // LANES):
            cols = slice(pair * LANES, (pair + 1) * LANES)
            weights = []
            reached = [[], []]
            for i in range(2):
                h = 2 * pair + i
                sides = []
                for d in range(2):
                    at = d * heads + h
                    mine = jnp.broadcast_to(cum[:, at : at + 1], (BLK, BLK))
                    gap = jnp.minimum(mine - cum_t[at : at + 1, :], 0.0)
                    dt = cum_t[2 * heads + at : 2 * heads + at + 1, :]
                    sides.append((jnp.exp2(gap) * (scores[d] * dt)).astype(BF16))
                    reached[d].append(mine)
                weights.append(jnp.concatenate(sides, axis=1))
            x_pair = jnp.concatenate([xf[:, cols], xb[:, cols]], axis=0)
            out = dot(jnp.concatenate(weights, axis=0), x_pair)
            total = jnp.where(first, out[:BLK], out[BLK:])
            for d in range(2):
                fade = jnp.exp2(jnp.where(first, reached[d][0], reached[d][1]))
                total += fade * dot(outs[d], starts[d, 0, :, cols])
                total += skip[d : d + 1, cols] * xs[d][:, cols].astype(F32)
            y[:, cols] = total

    def rows(width):
        return pl.BlockSpec((BLK, width), lambda b: (b, 0))

    return pl.pallas_call(
        body,
        grid=(blocks,),
        in_specs=[
            rows(channels),
            rows(channels),
            rows(states),
            rows(LANES),
            rows(LANES),
            pl.BlockSpec((2, 1, size, channels), lambda b: (0, b, 0, 0)),
            pl.BlockSpec(skip.shape, lambda b: (0, 0)),
        ],
        out_specs=rows(channels),
        out_shape=jax.ShapeDtypeStruct((tokens, channels), F32),
        compiler_params=mib(16),
        cost_estimate=pl.CostEstimate(flops=6_000_000_000, bytes_accessed=6 << 20, transcendentals=0),
        name="inside",
    )(xf, xb, bc, cum, cum_t, starts, skip)


def logs_of(ref, lead, size):
    rows = ref[lead + (slice(size, size + 16), slice(None))].astype(F32)
    return rows[0:1] + rows[1:2] + rows[2:3]


def messages(where, mine, theirs, groups):
    size, channels = mine.shape[1] - 16, mine.shape[2]

    def body(where, mine, theirs, *outs):
        group, second = where[1], where[2] == 1
        for d in range(2):
            own, other = logs_of(mine, (d,), size), logs_of(theirs, (d,), size)
            later = second if d == 0 else jnp.logical_not(second)
            scale_own = jnp.where(later, 1.0, jnp.exp2(other))
            scale_other = jnp.where(later, jnp.exp2(own), 1.0)
            total = own + other
            l1 = total.astype(BF16).astype(F32)
            l2 = (total - l1).astype(BF16).astype(F32)
            logs = jnp.concatenate([l1, l2, total - l1 - l2, jnp.zeros((13, channels), F32)], axis=0)
            state = scale_own * mine[d, :size, :].astype(F32) + scale_other * theirs[d, :size, :].astype(F32)
            state = state.astype(BF16)
            for k, out in enumerate(outs, 1):
                onward = group + k < groups

                @pl.when(onward if d == 0 else jnp.logical_not(onward))
                def _(out=out):
                    out[:size, :] = state
                    out[size:, :] = logs.astype(BF16)

    return pl.pallas_call(
        body,
        in_specs=[smem(), vmem(), vmem()],
        out_specs=[vmem()] * (groups - 1),
        out_shape=[jax.ShapeDtypeStruct(mine.shape[1:], BF16)] * (groups - 1),
        compiler_params=mib(16),
        cost_estimate=pl.CostEstimate(flops=1_000_000, bytes_accessed=2 << 20, transcendentals=0),
        name="messages",
    )(where, mine, theirs)


def entering(where, theirs, received, groups):
    size, channels = theirs.shape[1] - 16, theirs.shape[2]

    def body(where, theirs, *refs):
        got, out = refs[:-1], refs[-1]
        group, second = where[1], where[2] == 1
        for d in range(2):
            near = second if d == 0 else jnp.logical_not(second)
            log = jnp.where(near, logs_of(theirs, (d,), size), 0.0)
            state = jnp.where(near, 1.0, 0.0) * theirs[d, :size, :].astype(F32)
            for far in range(1, groups):
                ref = got[far - 1] if d == 0 else got[groups - far - 1]
                holds = far <= (group if d == 0 else groups - 1 - group)
                scale = jnp.where(holds, jnp.exp2(log), 0.0)
                state += scale * ref[:size, :].astype(F32)
                log = jnp.where(holds, log + logs_of(ref, (), size), log)
            out[d] = state.astype(BF16)

    return pl.pallas_call(
        body,
        in_specs=[smem()] + [vmem()] * (1 + len(received)),
        out_specs=vmem(),
        out_shape=jax.ShapeDtypeStruct((2, size, channels), BF16),
        compiler_params=mib(16),
        cost_estimate=pl.CostEstimate(flops=1_000_000, bytes_accessed=2 << 20, transcendentals=0),
        name="entering",
    )(where, theirs, *received)


def squares_of(packed):
    v = packed.astype(F32)
    return v + pltpu.roll(v, LANES // 2, 1)


def pack_squares(v):
    high = v.astype(BF16).astype(F32)
    lane = lax.broadcasted_iota(jnp.int32, v.shape, 1)
    return jnp.where(lane < LANES // 2, high, v - high).astype(BF16)


def finish(where, k, place, ring, y, bc, etot, gate, enter, spread, gain, w_out, last):
    tokens, channels = y.shape
    rows = tokens // ring
    half = rows // 2
    size = bc.shape[1] // 4
    width = w_out.shape[1]

    def body(where, y, bc, etot, gate, enter, spread, gain, w_out, *refs):
        outs, scaled = refs[:-1], refs[-1]
        square = jnp.zeros((rows, LANES), F32)
        for c in range(0, channels, 256):
            cols = slice(c, c + 256)
            total = y[:, cols]
            for d in range(2):
                c_rows = bc[:, (2 * d + 1) * size : (2 * d + 2) * size]
                total += dot(etot[...], spread[d, :, cols]) * dot(c_rows, enter[d, :, cols])
            gated = total * gate[:, cols]
            for t in range(0, 256, LANES):
                square += gated[:, t : t + LANES] * gated[:, t : t + LANES]
            scaled[:, cols] = (gated * gain[:, cols]).astype(BF16)
        square = square + pltpu.roll(square, LANES // 2, 1)
        if last:
            outs[1][...] = square
        else:
            packed = pack_squares(square)
            outs[0][:, width:] = packed[:half]
            outs[1][:, width:] = packed[half:]
        for c in range(0, width, 512):
            value = dot(scaled[...], w_out[:, c : c + 512])
            if last:
                outs[0][:, c : c + 512] = value
            else:
                outs[0][:, c : c + 512] = value[:half].astype(BF16)
                outs[1][:, c : c + 512] = value[half:].astype(BF16)

    def block(width):
        return pl.BlockSpec((rows, width), lambda i, w: (lax.rem(w[0] + k, ring), 0))

    def whole(shape):
        return pl.BlockSpec(shape, lambda i, w: (0,) * len(shape))

    if last:
        shapes = [((rows, width), F32), ((rows, LANES), F32)]
    else:
        shapes = [((half, width + LANES), BF16)] * 2
    return pl.pallas_call(
        body,
        grid_spec=pltpu.PrefetchScalarGridSpec(
            num_scalar_prefetch=1,
            grid=(1,),
            in_specs=[
                block(channels),
                block(bc.shape[1]),
                block(LANES),
                pl.BlockSpec((rows, channels), lambda i, w: (place, 0)),
                vmem(),
                vmem(),
                vmem(),
                vmem(),
            ],
            out_specs=[whole(s) for s, _ in shapes],
            scratch_shapes=[pltpu.VMEM((rows, channels), BF16)],
        ),
        out_shape=[jax.ShapeDtypeStruct(*s) for s in shapes],
        compiler_params=mib(16),
        cost_estimate=pl.CostEstimate(
            flops=2 * rows * channels * width, bytes_accessed=2 * channels * width, transcendentals=0
        ),
        name="finish",
    )(where, y, bc, etot, gate, enter, spread, gain, w_out)


def plus(value, got):
    width = value.shape[1] - LANES

    def body(value, got, out):
        out[:, :width] = (value[:, :width].astype(F32) + got[:, :width].astype(F32)).astype(BF16)
        out[:, width:] = pack_squares(squares_of(value[:, width:]) + squares_of(got[:, width:]))

    return pl.pallas_call(
        body,
        in_specs=[vmem()] * 2,
        out_specs=vmem(),
        out_shape=jax.ShapeDtypeStruct(value.shape, BF16),
        compiler_params=mib(8),
        name="plus",
    )(value, got)


def normalize(value, square, halves, channels):
    rows, width = value.shape
    half = rows // 2
    each = [len(h) for h in halves]

    def body(value, square, *refs):
        ins, out = refs[:-1], refs[-1]
        for i, group in enumerate((ins[: each[0]], ins[each[0] :])):
            part = slice(i * half, (i + 1) * half)
            total, squares = value[part, :], square[part, :]
            for ref in group:
                total = total + ref[:, :width].astype(F32)
                squares = squares + squares_of(ref[:, width:])
            mean = jnp.sum(squares, axis=1, keepdims=True) / (2.0 * channels)
            out[part, :] = (total * lax.rsqrt(mean + 1e-05)).astype(BF16)

    return pl.pallas_call(
        body,
        in_specs=[vmem()] * (2 + sum(each)),
        out_specs=vmem(),
        out_shape=jax.ShapeDtypeStruct(value.shape, BF16),
        compiler_params=mib(8),
        name="normalize",
    )(value, square, *halves[0], *halves[1])


def ring_pairs(count, step):
    return [(i, (i + step) % count) for i in range(count)]


def per_device(
    tokens,
    w_gate,
    w_value,
    w_state_proj,
    w_step,
    step_bias,
    decay_rate,
    conv_taps,
    skip_gain,
    norm_gain,
    w_out,
):
    ring, frames = lax.axis_size("row"), lax.axis_size("frame")
    row, frame = lax.axis_index("row"), lax.axis_index("frame")
    channels, heads = w_gate.shape[1], step_bias.shape[1]
    span = 2 if frames % 2 == 0 else 1
    groups = frames // span
    where = jnp.stack([row, frame // span, frame % span]).astype(jnp.int32)
    own = tokens.reshape(-1, tokens.shape[2])
    rows = own.shape[0]
    far = ring // 2
    edge = 8

    def up(v):
        return lax.ppermute(v, "row", ring_pairs(ring, 1))

    def down(v):
        return lax.ppermute(v, "row", ring_pairs(ring, -1))

    first, second, ends = split(where, own, ring, edge)
    arrived = []
    from_below, from_above = [first, second], [second, first]
    for hop in range(1, far + 1):
        with jax.named_scope("lead"):
            a, c = up(from_below[0]), down(from_above[0])
        if 2 * hop == ring:
            arrived.append([a, c])
        else:
            with jax.named_scope("rest"):
                b, d = up(from_below[1]), down(from_above[1])
            from_below, from_above = [a, b], [c, d]
            arrived.append([a, b, d, c])
    bounds = []
    for j in range(ring):
        pairs = [(f * ring + ring - 1, (f + 1) * ring + (ring - 1 + j) % ring) for f in range(frames - 1)]
        pairs += [((f + 1) * ring, f * ring + j) for f in range(frames - 1)]
        bounds.append(lax.ppermute(ends, ("frame", "row"), pairs))

    spread, small_rows, skip = prepare(step_bias, decay_rate, skip_gain, channels)
    gain = norm_gain.reshape(1, -1)
    steps = jnp.swapaxes(w_step, 1, 2).reshape(-1, w_step.shape[1])

    order, projected = [0], [project(where, [own], bounds, w_value, w_state_proj, steps)]
    for hop, pieces in enumerate(arrived, 1):
        order += [ring - hop, hop] if len(pieces) == 4 else [hop]
        projected.append(project(where, pieces, [], w_value, w_state_proj, steps))
    xs, bcs, sts = zip(*projected)
    place = {k: j for j, k in enumerate(order)}

    xf, xb, bc, cum, cum_t, etot, starts, pack = frame_states(
        where, order, rows, edge, xs, bcs, sts, conv_taps, small_rows, spread, heads
    )

    if span == 2:
        theirs = lax.ppermute(pack, "frame", [(i, i ^ 1) for i in range(frames)])
    else:
        theirs = jnp.zeros_like(pack)
    received = []
    if groups > 1:
        sends = messages(where, pack, theirs, groups)
        for k, send in enumerate(sends, 1):
            pairs = [
                (g * span + s, (g + k) % groups * span + s) for g in range(groups) for s in range(span)
            ]
            received.append(lax.ppermute(send, "frame", pairs))
    y = inside(xf, xb, bc, cum, cum_t, starts, skip, heads)
    gate = gates([own] + [p for pieces in arrived for p in pieces], w_gate)
    enter = entering(where, theirs, received, groups)

    def block(k):
        return finish(
            where, k, place[k], ring, y, bc, etot, gate, enter, spread, gain, w_out, k == 0
        )

    up_a = up_b = down_a = down_b = None
    for hop in range(far, 0, -1):
        if 2 * hop == ring:
            a, b = block(hop)
            up_a, down_b = up(a), down(b)
            continue
        (above_a, above_b), (below_a, below_b) = block(hop), block(ring - hop)
        up_b = up(above_b if up_b is None else plus(above_b, up_b))
        down_a = down(below_a if down_a is None else plus(below_a, down_a))
        up_a = up(above_a if up_a is None else plus(above_a, up_a))
        down_b = down(below_b if down_b is None else plus(below_b, down_b))
    value, square = block(0)
    halves = [[v for v in pair if v is not None] for pair in ((up_a, down_a), (up_b, down_b))]
    return normalize(value, square, halves, channels * ring).reshape(tokens.shape)


def solution(mesh):
    return jax.shard_map(
        per_device,
        mesh=mesh,
        in_specs=(
            P("frame", "row", None),
            P(None, "row"),
            P(None, "row"),
            P(),
            P(None, None, "row"),
            P(None, "row"),
            P(None, "row"),
            P(None, None, "row"),
            P(None, "row"),
            P("row"),
            P("row", None),
        ),
        out_specs=P("frame", "row", None),
        check_vma=False,
    )
```

```python
import math

import jax
import jax.numpy as jnp
from jax import lax
from jax.experimental import pallas as pl
from jax.experimental.pallas import tpu as pltpu
from jax.sharding import PartitionSpec as P


HEAD_DIM = 64
LANES = 128
LOGS = 8
SPLIT = 20_000_000_000
LOG2E = 1.0 / math.log(2.0)
F32 = jnp.float32
BF16 = jnp.bfloat16


def mib(size):
    return pltpu.CompilerParams(vmem_limit_bytes=size << 20)


def vmem():
    return pl.BlockSpec(memory_space=pltpu.VMEM)


def smem():
    return pl.BlockSpec(memory_space=pltpu.SMEM)


def dot(a, b):
    return jnp.dot(a, b, preferred_element_type=F32)


def silu(v):
    return v / (1.0 + jnp.exp(-v))


def two_parts(v, stride):
    high = v.astype(BF16).astype(F32)
    return (high + pltpu.roll(v - high, stride, 1)).astype(BF16)


def split(where, own, ring, edge):
    rows, depth = own.shape
    half = rows // 2

    def body(where, own, a, b, outer):
        a[...] = own[:half, :]
        b[...] = own[half:, :]

        @pl.when(where[0] == ring - 1)
        def _():
            outer[...] = own[rows - edge :, :]

        @pl.when(where[0] != ring - 1)
        def _():
            outer[...] = own[:edge, :]

    shapes = [(half, depth), (half, depth), (edge, depth)]
    return pl.pallas_call(
        body,
        in_specs=[smem(), vmem()],
        out_specs=[vmem()] * 3,
        out_shape=[jax.ShapeDtypeStruct(s, BF16) for s in shapes],
        compiler_params=mib(8),
        cost_estimate=pl.CostEstimate(flops=SPLIT, bytes_accessed=2 << 20, transcendentals=0),
        name="split",
    )(where, own)


def prepare(step_bias, decay_rate, skip_gain, channels):
    heads = step_bias.shape[1]
    rest = LANES - 2 * heads

    def body(bias, rate, skip, spread, rows, skips):
        lane = lax.broadcasted_iota(jnp.int32, (LANES, channels), 0)
        head = lax.shift_right_logical(
            lax.broadcasted_iota(jnp.int32, (LANES, channels), 1), HEAD_DIM.bit_length() - 1
        )
        for d in range(2):
            hit = (lane == head + d * heads) | (lane == head + (2 + d) * heads)
            spread[d] = jnp.where(hit, 1.0, 0.0).astype(BF16)
        zeros = jnp.zeros((1, rest), F32)
        for at, ref in enumerate((bias, rate)):
            rows[at : at + 1, :] = jnp.concatenate([ref[0:1, :], ref[1:2, :], zeros], axis=1)
        pieces = jnp.concatenate([skip[...], jnp.zeros((2, LANES - heads), F32)], axis=1)
        p1 = pieces.astype(BF16).astype(F32)
        p2 = (pieces - p1).astype(BF16).astype(F32)
        p3 = pieces - p1 - p2
        stack = jnp.concatenate([p1, p2, p3, jnp.zeros((10, LANES), F32)], axis=0).astype(BF16)
        wide = dot(stack, spread[0])
        skips[...] = wide[0:2] + wide[2:4] + wide[4:6]

    shapes = [((2, LANES, channels), BF16), ((2, LANES), F32), ((2, channels), F32)]
    return pl.pallas_call(
        body,
        in_specs=[vmem()] * 3,
        out_specs=[vmem()] * 3,
        out_shape=[jax.ShapeDtypeStruct(*s) for s in shapes],
        compiler_params=mib(8),
        name="prepare",
    )(step_bias, decay_rate, skip_gain)


def gather(refs, stacked):
    at = 0
    for ref in refs:
        stacked[at : at + ref.shape[0], :] = ref[...]
        at += ref.shape[0]


def conv_of(window, taps, backward, count):
    reach = taps.shape[0] - 1
    total = 0.0
    for j in range(reach + 1):
        start = reach - j if backward else j
        total = total + taps[j : j + 1] * window[start : start + count]
    return silu(total)


def block_states(pieces, bounds, where, w_value, w_state, w_step, taps, small_rows, heads):
    rows, depth = sum(p.shape[0] for p in pieces), pieces[0].shape[1]
    channels, states, steps = w_value.shape[1], w_state.shape[1], w_step.shape[0]
    size = states // 4
    reach = taps.shape[1] - 1
    count, around = len(pieces), len(bounds)
    pad = 8
    total = rows + (2 * pad if around else 0)

    def body(where, *refs):
        src, refs = refs[:count], refs[count:]
        edges, refs = refs[:around], refs[around:]
        wv, ws, wt, taps, small = refs[:5]
        xf, xb, ends, bc, b_t, cum_out, cum_t, reached, fade, last_out = refs[5:15]
        stacked, sx = refs[-2:]
        gather(src, stacked)
        for j, ref in enumerate(edges):

            @pl.when(lax.rem(where[0] + 1, around) == j)
            def _(ref=ref):
                stacked[rows : rows + pad, :] = ref[...]

            @pl.when(where[0] == j)
            def _(ref=ref):
                stacked[rows + pad :, :] = ref[...]

        sx[:pad, :] = jnp.zeros((pad, channels), F32)
        sx[pad + rows :, :] = jnp.zeros((pad, channels), F32)

        def conv(n):
            for at in range(n, n + 256, LANES):
                cols = slice(at, at + LANES)
                ahead, behind = taps[0, :, cols], taps[1, :, cols]
                for base in range(pad, pad + rows, 64):
                    views = {o: sx[base + o : base + o + 64, cols] for o in range(-reach, reach + 1)}
                    f = sum(ahead[j : j + 1] * views[j - reach] for j in range(reach + 1))
                    b = sum(behind[j : j + 1] * views[reach - j] for j in range(reach + 1))
                    xf[base - pad : base - pad + 64, cols] = silu(f).astype(BF16)
                    xb[base - pad : base - pad + 64, cols] = silu(b).astype(BF16)

        for n in range(0, channels, 256):
            cols = slice(n, n + 256)
            x = dot(stacked[...], wv[:, cols]).astype(BF16)
            sx[pad : pad + rows, cols] = x[:rows].astype(F32)
            ends[:pad, cols] = x[:pad]
            ends[pad : 2 * pad, cols] = x[rows - pad : rows]
            if around:
                ends[2 * pad :, cols] = x[rows:]
            if n:
                conv(n - 256)
        raw = lax.dot_general(
            stacked[:rows, :], wt[...], (((1,), (1,)), ((), ())), preferred_element_type=F32
        )
        raw = jnp.concatenate(
            [raw.astype(BF16).astype(F32), jnp.zeros((rows, LANES - steps), F32)], axis=1
        )
        for n in range(0, states, 256):
            bc[:, n : n + 256] = dot(stacked[:rows, :], ws[:, n : n + 256]).astype(BF16)
        conv(channels - 256)

        lane = lax.broadcasted_iota(jnp.int32, (rows, LANES), 1)
        used, forward = lane < 2 * heads, lane < heads
        low_row, low_col = (lax.broadcasted_iota(jnp.int32, (rows, rows), d) for d in (0, 1))
        both = jnp.concatenate(
            [
                jnp.where(low_row >= low_col, 1.0, 0.0).astype(BF16),
                jnp.where(low_row <= low_col, 1.0, 0.0).astype(BF16),
            ],
            axis=0,
        )
        v = raw + small[0:1, :]
        dt = jnp.maximum(v, 0.0) + jnp.log1p(jnp.exp(-jnp.abs(v)))
        dt = jnp.where(used, dt, 0.0)
        a = -dt * small[1:2, :] * LOG2E
        a1 = a.astype(BF16).astype(F32)
        a2 = (a - a1).astype(BF16).astype(F32)
        a3 = a - a1 - a2
        parts = a1 + pltpu.roll(a2, 2 * heads, 1) + pltpu.roll(a3, 4 * heads, 1)
        sums = dot(both, parts.astype(BF16))
        sums = pltpu.roll(sums, LANES - 4 * heads, 1) + pltpu.roll(sums, LANES - 2 * heads, 1) + sums
        cum = jnp.where(used, jnp.where(forward, sums[:rows], sums[rows:]), 0.0)
        last = jnp.where(forward[:1], cum[rows - 1 :], cum[:1])
        last_out[...] = jnp.broadcast_to(last, last_out.shape)
        cum_out[...] = cum
        cum_t[...] = (cum + pltpu.roll(dt, 2 * heads, 1)).T
        reached[...] = two_parts(jnp.where(used, jnp.exp2(cum), 0.0), 2 * heads)
        fade[...] = jnp.exp2(last - cum) * dt
        for d in range(2):
            b_t[d] = bc[:, d * 2 * size : (2 * d + 1) * size].astype(F32).T.astype(BF16)

    shapes = [
        ((rows, channels), BF16),
        ((rows, channels), BF16),
        ((4 * pad if around else 2 * pad, channels), BF16),
        ((rows, states), BF16),
        ((2, size, rows), BF16),
        ((rows, LANES), F32),
        ((LANES, rows), F32),
        ((rows, LANES), BF16),
        ((rows, LANES), F32),
        ((8, LANES), F32),
    ]
    width = channels + states + LANES
    return pl.pallas_call(
        body,
        in_specs=[smem()] + [vmem()] * (count + around + 5),
        out_specs=[vmem()] * len(shapes),
        out_shape=[jax.ShapeDtypeStruct(*s) for s in shapes],
        scratch_shapes=[
            pltpu.VMEM((total, depth), BF16),
            pltpu.VMEM((rows + 2 * pad, channels), F32),
        ],
        compiler_params=mib(16),
        cost_estimate=pl.CostEstimate(
            flops=3 * total * depth * width, bytes_accessed=2 * depth * width, transcendentals=0
        ),
        name="block_states",
    )(where, *pieces, *bounds, w_value, w_state, w_step, taps, small_rows)


def frame_logs(where, lasts, ring):
    at = [lax.rem(where[0] + k, ring) for k in range(ring)]
    rows = [ref[0:1, :] for ref in lasts]

    def between(low, high):
        out = jnp.zeros_like(rows[0])
        for place, row in zip(at, rows):
            out += jnp.where(jnp.logical_and(place > low, place < high), row, 0.0)
        return out

    return at, rows, between


def spread_rows(rows, heads, spread):
    lane = lax.broadcasted_iota(jnp.int32, rows[0].shape, 1)
    rows = [jnp.where(lane < 2 * heads, jnp.exp2(r), 0.0) for r in rows]
    short = -len(rows) % 8
    if short:
        rows.append(jnp.zeros((short, LANES), F32))
    packed = two_parts(jnp.concatenate(rows, axis=0), 2 * heads)
    return [dot(packed, spread[d]) for d in range(2)]


def combine(where, xfs, xbs, ends, b_ts, fades, lasts, taps, spread, heads):
    ring = len(xfs)
    rows, channels = xfs[0].shape
    size = b_ts[0].shape[1]
    pad = 8
    reach = taps.shape[1] - 1

    def body(where, *refs):
        xf, xb, ends, b_t, fades, lasts = (refs[i * ring : (i + 1) * ring] for i in range(6))
        taps, spread, pack, fixed, qs, carried, b_all = refs[6 * ring :]
        at, logs, between = frame_logs(where, lasts, ring)
        forward = lax.broadcasted_iota(jnp.int32, logs[0].shape, 1) < heads
        for k in range(ring):
            later = jnp.where(forward, between(at[k], ring), between(-1, at[k]))
            qs[k * rows : (k + 1) * rows, :] = two_parts(fades[k][...] * jnp.exp2(later), 2 * heads)
            for d in range(2):
                b_all[d, :, k * rows : (k + 1) * rows] = b_t[k][d]
            first, final = at[k] == 0, at[k] == ring - 1
            below, above = ends[(k - 1) % ring], ends[(k + 1) % ring]
            for n in range(0, channels, 256):
                cols = slice(n, n + 256)
                own = ends[k][: 2 * pad, cols].astype(F32)
                before = jnp.where(first, ends[1][2 * pad : 3 * pad, cols], below[pad : 2 * pad, cols])
                after = jnp.where(final, ends[1][3 * pad :, cols], above[:pad, cols])
                window = jnp.concatenate([before.astype(F32), own[:pad]], axis=0)
                fixed[k, :pad, cols] = conv_of(
                    window[pad - reach :], taps[0, :, cols], False, pad
                ).astype(BF16)
                window = jnp.concatenate([own[pad:], after.astype(F32)], axis=0)
                fixed[k, pad:, cols] = conv_of(
                    window[: pad + reach], taps[1, :, cols], True, pad
                ).astype(BF16)
        total = sum(logs[1:], logs[0])
        l1 = total.astype(BF16).astype(F32)
        l2 = (total - l1).astype(BF16).astype(F32)
        three = jnp.concatenate([l1, l2, total - l1 - l2, jnp.zeros((LOGS - 3, LANES), F32)], axis=0)
        for d in range(2):
            pack[d, size:, :] = dot(three.astype(BF16), spread[d]).astype(BF16)
            for n in range(0, channels, 256):
                cols = slice(n, n + 256)
                scale = dot(qs[...], spread[d, :, cols])
                for k in range(ring):
                    x = patched((xf, xb)[d][k], fixed, k, cols, pad, d)
                    part = slice(k * rows, (k + 1) * rows)
                    carried[part, :] = (scale[part] * x.astype(F32)).astype(BF16)
                pack[d, :size, cols] = dot(b_all[d], carried[...]).astype(BF16)

    return pl.pallas_call(
        body,
        in_specs=[smem()] + [vmem()] * (6 * ring + 2),
        out_specs=[vmem()] * 2,
        out_shape=[
            jax.ShapeDtypeStruct((2, size + LOGS, channels), BF16),
            jax.ShapeDtypeStruct((ring, 2 * pad, channels), BF16),
        ],
        scratch_shapes=[
            pltpu.VMEM((ring * rows, LANES), BF16),
            pltpu.VMEM((ring * rows, 256), BF16),
            pltpu.VMEM((2, size, ring * rows), BF16),
        ],
        compiler_params=mib(16),
        cost_estimate=pl.CostEstimate(flops=2_000_000_000, bytes_accessed=4 << 20, transcendentals=0),
        name="combine",
    )(where, *xfs, *xbs, *ends, *b_ts, *fades, *lasts, taps, spread)


def patched(x, fixed, k, cols, pad, d):
    rows = x.shape[0]
    if d == 0:
        return jnp.concatenate([fixed[k, :pad, cols], x[pad:, cols]], axis=0)
    return jnp.concatenate([x[: rows - pad, cols], fixed[k, pad:, cols]], axis=0)


def starts_of(where, xfs, xbs, fixed, b_ts, fades, lasts, spread, heads):
    ring = len(xfs)
    rows, channels = xfs[0].shape
    size = b_ts[0].shape[1]
    pad = fixed.shape[1] // 2

    def body(where, *refs):
        xf, xb, b_t, fades, lasts = (refs[i * ring : (i + 1) * ring] for i in range(5))
        fixed, spread, starts, fades_out, qs = refs[5 * ring :]
        at, logs, between = frame_logs(where, lasts, ring)
        forward = lax.broadcasted_iota(jnp.int32, logs[0].shape, 1) < heads
        fade = spread_rows(
            [jnp.where(forward, between(-1, p), between(p, ring)) for p in at], heads, spread
        )
        for d in range(2):
            fades_out[d] = fade[d]
        for k in range(ring):
            qs[k * rows : (k + 1) * rows, :] = two_parts(fades[k][...], 2 * heads)
        weights = [
            spread_rows(
                [
                    jnp.where(forward, between(at[k], at[j]), between(at[j], at[k]))
                    for k in range(ring)
                ],
                heads,
                spread,
            )
            for j in range(ring)
        ]
        for d in range(2):
            for n in range(0, channels, 256):
                cols = slice(n, n + 256)
                scale = dot(qs[...], spread[d, :, cols])
                for k in range(ring):
                    x = patched((xf, xb)[d][k], fixed, k, cols, pad, d)
                    part = slice(k * rows, (k + 1) * rows)
                    added = dot(b_t[k][d], (scale[part] * x.astype(F32)).astype(BF16))
                    for j in range(ring):
                        if j == k:
                            continue
                        before = at[k] < at[j] if d == 0 else at[k] > at[j]
                        term = jnp.where(before, weights[j][d][k : k + 1, cols], 0.0) * added
                        if k == (1 if j == 0 else 0):
                            starts[j, d, :, cols] = term
                        else:
                            starts[j, d, :, cols] += term

    return pl.pallas_call(
        body,
        in_specs=[smem()] + [vmem()] * (5 * ring + 2),
        out_specs=[vmem()] * 2,
        out_shape=[
            jax.ShapeDtypeStruct((ring, 2, size, channels), F32),
            jax.ShapeDtypeStruct((2, ring + -ring % 8, channels), F32),
        ],
        scratch_shapes=[pltpu.VMEM((ring * rows, LANES), BF16)],
        compiler_params=mib(16),
        cost_estimate=pl.CostEstimate(flops=1_200_000_000, bytes_accessed=8 << 20, transcendentals=0),
        name="starts",
    )(where, *xfs, *xbs, *b_ts, *fades, *lasts, fixed, spread)


def inside(k, xf, xb, fixed, bc, cum, cum_t, skip, heads):
    rows, channels = xf.shape
    size = bc.shape[1] // 4

    pad = fixed.shape[1] // 2

    def body(xf, xb, fixed, bc, cum, cum_t, skip, y):
        row, col = (lax.broadcasted_iota(jnp.int32, (rows, rows), d) for d in (0, 1))
        first = lax.broadcasted_iota(jnp.int32, (rows, LANES), 1) < HEAD_DIM
        scores = []
        for d in range(2):
            b_rows = bc[:, 2 * d * size : (2 * d + 1) * size]
            c_rows = bc[:, (2 * d + 1) * size : (2 * d + 2) * size]
            s = lax.dot_general(
                c_rows, b_rows, (((1,), (1,)), ((), ())), preferred_element_type=F32
            )
            scores.append(jnp.where(row >= col if d == 0 else row <= col, s, 0.0))
        for pair in range(channels // LANES):
            cols = slice(pair * LANES, (pair + 1) * LANES)
            weights = []
            for h in range(pair * (LANES // HEAD_DIM), (pair + 1) * (LANES // HEAD_DIM)):
                sides = []
                for d in range(2):
                    at = d * heads + h
                    gap = jnp.minimum(cum[:, at : at + 1] - cum_t[at : at + 1, :], 0.0)
                    dt = cum_t[2 * heads + at : 2 * heads + at + 1, :]
                    sides.append((jnp.exp2(gap) * (scores[d] * dt)).astype(BF16))
                weights.append(jnp.concatenate(sides, axis=1))
            sides = [patched(x, fixed, k, cols, pad, d) for d, x in enumerate((xf, xb))]
            x_pair = jnp.concatenate(sides, axis=0)
            out = dot(jnp.concatenate(weights, axis=0), x_pair)
            total = jnp.where(first, out[:rows], out[rows:])
            total += skip[0:1, cols] * sides[0].astype(F32)
            total += skip[1:2, cols] * sides[1].astype(F32)
            y[:, cols] = total

    return pl.pallas_call(
        body,
        in_specs=[vmem()] * 7,
        out_specs=vmem(),
        out_shape=jax.ShapeDtypeStruct((rows, channels), F32),
        compiler_params=mib(12),
        cost_estimate=pl.CostEstimate(flops=1_200_000_000, bytes_accessed=2 << 20, transcendentals=0),
        name="inside",
    )(xf, xb, fixed, bc, cum, cum_t, skip)


def gates(pieces, w_gate):
    rows, depth = sum(p.shape[0] for p in pieces), pieces[0].shape[1]
    channels, count = w_gate.shape[1], len(pieces)

    def body(*refs):
        wg, gate, block = refs[count:]
        gather(refs[:count], block)
        for n in range(0, channels, 256):
            raw = dot(block[...], wg[:, n : n + 256]).astype(BF16)
            gate[:, n : n + 256] = silu(raw.astype(F32))

    return pl.pallas_call(
        body,
        in_specs=[vmem()] * (count + 1),
        out_specs=vmem(),
        out_shape=jax.ShapeDtypeStruct((rows, channels), F32),
        scratch_shapes=[pltpu.VMEM((rows, depth), BF16)],
        compiler_params=mib(12),
        cost_estimate=pl.CostEstimate(
            flops=2 * rows * depth * channels, bytes_accessed=2 * depth * channels, transcendentals=0
        ),
        name="gates",
    )(*pieces, w_gate)


def log_rows(rows):
    rows = rows.astype(F32)
    return rows[0:1] + rows[1:2] + rows[2:3]


def messages(where, mine, theirs, groups, parts):
    size, channels = mine.shape[1] - LOGS, mine.shape[2]
    width = channels // parts

    def body(where, mine, theirs, *outs):
        group, second = where[1], where[2] == 1
        cols = pl.ds(pl.multiple_of(where[2] * width, LANES), width)
        for d in range(2):
            own, other = log_rows(mine[d, size:, cols]), log_rows(theirs[d, size:, cols])
            later = second if d == 0 else jnp.logical_not(second)
            scale_own = jnp.where(later, 1.0, jnp.exp2(other))
            scale_other = jnp.where(later, jnp.exp2(own), 1.0)
            total = own + other
            l1 = total.astype(BF16).astype(F32)
            l2 = (total - l1).astype(BF16).astype(F32)
            logs = jnp.concatenate(
                [l1, l2, total - l1 - l2, jnp.zeros((LOGS - 3, width), F32)], axis=0
            ).astype(BF16)
            state = scale_own * mine[d, :size, cols].astype(F32)
            state = (state + scale_other * theirs[d, :size, cols].astype(F32)).astype(BF16)
            for k, out in enumerate(outs, 1):
                onward = group + k < groups

                @pl.when(onward if d == 0 else jnp.logical_not(onward))
                def _(out=out):
                    out[:size, :] = state
                    out[size:, :] = logs

    return pl.pallas_call(
        body,
        in_specs=[smem(), vmem(), vmem()],
        out_specs=[vmem()] * (groups - 1),
        out_shape=[jax.ShapeDtypeStruct((size + LOGS, width), BF16)] * (groups - 1),
        compiler_params=mib(16),
        cost_estimate=pl.CostEstimate(flops=1_000_000, bytes_accessed=2 << 20, transcendentals=0),
        name="messages",
    )(where, mine, theirs)


def entering(where, received, groups):
    size, width = received[0].shape[0] - LOGS, received[0].shape[1]

    def body(where, *refs):
        got, out = refs[:-1], refs[-1]
        group = where[1]
        for d in range(2):
            log = jnp.zeros((1, width), F32)
            state = jnp.zeros((size, width), F32)
            for far in range(1, groups):
                ref = got[far - 1] if d == 0 else got[groups - far - 1]
                holds = far <= (group if d == 0 else groups - 1 - group)
                scale = jnp.where(holds, jnp.exp2(log), 0.0)
                state += scale * ref[:size, :].astype(F32)
                log = jnp.where(holds, log + log_rows(ref[size:, :]), log)
            out[d] = state.astype(BF16)

    return pl.pallas_call(
        body,
        in_specs=[smem()] + [vmem()] * len(received),
        out_specs=vmem(),
        out_shape=jax.ShapeDtypeStruct((2, size, width), BF16),
        compiler_params=mib(16),
        cost_estimate=pl.CostEstimate(flops=1_000_000, bytes_accessed=2 << 20, transcendentals=0),
        name="entering",
    )(where, *received)


SUB = 16


def pack_squares(row):
    high = row.astype(BF16).astype(F32)
    return jnp.concatenate([high, row - high, jnp.zeros((SUB - 2, LANES), F32)], axis=0).astype(BF16)


def squares_of(packed):
    v = packed.astype(F32)
    return v[0:1] + v[1:2]


def finish(where, k, y, bc, reached, gate, starts, fades, theirs, mine, other, spread, gain, w_out):
    rows, channels = y.shape
    size = bc.shape[1] // 4
    width = w_out.shape[1]
    half = rows // 2
    last = k == 0
    part = mine.shape[2]
    step = min(256, part)
    across = width // LANES
    count = half // SUB * across

    def body(where, y, bc, reached, gate, starts, fades, theirs, mine, other, spread, gain, w_out, *refs):
        outs, scaled = refs[:-1], refs[-1]
        second = where[2] == 1
        square = jnp.zeros((rows, LANES), F32)
        for n in range(0, channels, step):
            cols = slice(n, n + step)
            total = y[:, cols]
            for d in range(2):
                c_rows = bc[:, (2 * d + 1) * size : (2 * d + 2) * size]
                near = second if d == 0 else jnp.logical_not(second)
                at = slice(n % part, n % part + step)
                enter = jnp.where(where[2] == n // part, mine[d, :, at], other[d, :, at]).astype(F32)
                log = jnp.where(near, log_rows(theirs[d, size:, cols]), 0.0)
                enter = jnp.exp2(log) * enter
                enter += jnp.where(near, theirs[d, :size, cols].astype(F32), 0.0)
                state = starts[0, d, :, cols] + fades[d, k : k + 1, cols] * enter
                total += dot(reached[...], spread[d, :, cols]) * dot(c_rows, state.astype(BF16))
            gated = total * gate[:, cols]
            for t in range(0, step, LANES):
                square += gated[:, t : t + LANES] * gated[:, t : t + LANES]
            scaled[:, cols] = (gated * gain[:, cols]).astype(BF16)
        sums = jnp.broadcast_to(jnp.sum(square, axis=1, keepdims=True), (rows, LANES))
        row = sums.T[0:1, :]
        if last:
            outs[1][...] = jnp.broadcast_to(row, (SUB, rows))
        else:
            for out in outs:
                out[count] = pack_squares(row)
        for n in range(0, width, 256):
            value = dot(scaled[...], w_out[:, n : n + 256])
            if last:
                outs[0][:, n : n + 256] = value
                continue
            value = value.astype(BF16)
            for i in range(rows // SUB):
                for j in range(0, 256, LANES):
                    tile = value[i * SUB : (i + 1) * SUB, j : j + LANES]
                    place = i % (half // SUB) * across + (n + j) // LANES
                    outs[i * SUB // half][place] = tile

    if last:
        shapes = [((rows, width), F32), ((SUB, rows), F32)]
    else:
        shapes = [((count + 1, SUB, LANES), BF16)] * 2
    specs = [smem()] + [vmem()] * 12
    specs[5] = pl.BlockSpec((1,) + starts.shape[1:], lambda i: (k, 0, 0, 0))
    return pl.pallas_call(
        body,
        grid=(1,),
        in_specs=specs,
        out_specs=[vmem()] * len(shapes),
        out_shape=[jax.ShapeDtypeStruct(*s) for s in shapes],
        scratch_shapes=[pltpu.VMEM((rows, channels), BF16)],
        compiler_params=mib(16),
        cost_estimate=pl.CostEstimate(
            flops=2 * rows * channels * width, bytes_accessed=2 * channels * width, transcendentals=0
        ),
        name="finish",
    )(where, y, bc, reached, gate, starts, fades, theirs, mine, other, spread, gain, w_out)


def plus(value, got):
    count = value.shape[0] - 1

    def body(value, got, out):
        for n in range(0, count, 8):
            part = slice(n, min(n + 8, count))
            out[part] = (value[part].astype(F32) + got[part].astype(F32)).astype(BF16)
        out[count] = pack_squares(squares_of(value[count]) + squares_of(got[count]))

    return pl.pallas_call(
        body,
        in_specs=[vmem()] * 2,
        out_specs=vmem(),
        out_shape=jax.ShapeDtypeStruct(value.shape, BF16),
        compiler_params=mib(8),
        name="plus",
    )(value, got)


def normalize(value, square, halves, channels):
    rows, width = value.shape
    half = rows // 2
    across = width // LANES
    count = half // SUB * across
    each = [len(h) for h in halves]

    def body(value, square, *refs):
        ins, out = refs[:-1], refs[-1]
        lane = lax.broadcasted_iota(jnp.int32, (1, rows), 1)
        groups = (ins[: each[0]], ins[each[0] :])
        sums = square[0:1, :]
        for i, group in enumerate(groups):
            for ref in group:
                got = squares_of(ref[count])
                sums = sums + jnp.where((lane >= half) == (i == 1), got, 0.0)
        scale = lax.rsqrt(sums / channels + 1e-05)
        scale = jnp.broadcast_to(scale, (LANES, rows)).T
        for i in range(rows // SUB):
            group = groups[i * SUB // half]
            for j in range(across):
                at = (slice(i * SUB, (i + 1) * SUB), slice(j * LANES, (j + 1) * LANES))
                total = value[at]
                for ref in group:
                    total = total + ref[i % (half // SUB) * across + j].astype(F32)
                out[at] = (total * scale[at[0], :]).astype(BF16)

    return pl.pallas_call(
        body,
        in_specs=[vmem()] * (2 + sum(each)),
        out_specs=vmem(),
        out_shape=jax.ShapeDtypeStruct(value.shape, BF16),
        compiler_params=mib(8),
        name="normalize",
    )(value, square, *halves[0], *halves[1])


def ring_pairs(count, step):
    return [(i, (i + step) % count) for i in range(count)]


def layer(
    tokens,
    w_gate,
    w_value,
    w_state_proj,
    w_step,
    step_bias,
    decay_rate,
    conv_taps,
    skip_gain,
    norm_gain,
    w_out,
):
    ring, frames = lax.axis_size("row"), lax.axis_size("frame")
    row, frame = lax.axis_index("row"), lax.axis_index("frame")
    channels, heads = w_gate.shape[1], step_bias.shape[1]
    span = 2 if frames % 2 == 0 else 1
    groups = frames // span
    where = jnp.stack([row, frame // span, frame % span]).astype(jnp.int32)
    own = tokens.reshape(-1, tokens.shape[2])
    far = ring // 2
    edge = 8
    end = ring - 1

    def up(v):
        return lax.ppermute(v, "row", ring_pairs(ring, 1))

    def down(v):
        return lax.ppermute(v, "row", ring_pairs(ring, -1))

    first, second, outer = split(where, own, ring, edge)
    pieces = {0: [first, second]}
    order = [0]
    from_below, from_above = [first, second], [second, first]
    for hop in range(1, far + 1):
        a, c = up(from_below[0]), down(from_above[0])
        if 2 * hop == ring:
            pieces[hop] = [a, c]
            order.append(hop)
        else:
            b, d = up(from_below[1]), down(from_above[1])
            from_below, from_above = [a, b], [c, d]
            pieces[ring - hop], pieces[hop] = [a, b], [d, c]
            order += [ring - hop, hop]
    bounds = []
    for j in range(ring):
        pairs = [(f * ring + end, (f + 1) * ring + (end + j) % ring) for f in range(frames - 1)]
        pairs += [((f + 1) * ring, f * ring + j) for f in range(frames - 1)]
        bounds.append(lax.ppermute(outer, ("frame", "row"), pairs))

    steps = jnp.swapaxes(w_step, 1, 2).reshape(-1, w_step.shape[1])
    spread, small_rows, skip = prepare(step_bias, decay_rate, skip_gain, channels)
    gain = norm_gain.reshape(1, -1)

    blocks = {}
    for k in order:
        blocks[k] = block_states(
            pieces[k],
            bounds if k == 1 else [],
            where,
            w_value,
            w_state_proj,
            steps,
            conv_taps,
            small_rows,
            heads,
        )
    xfs, xbs, ends, bcs, b_ts, cums, cum_ts, reached, fading, lasts = (
        [blocks[k][i] for k in range(ring)] for i in range(len(blocks[0]))
    )
    pack, fixed = combine(where, xfs, xbs, ends, b_ts, fading, lasts, conv_taps, spread, heads)

    if span == 2:
        swap = [(i, i ^ 1) for i in range(frames)]
        theirs = lax.ppermute(pack, "frame", swap)
    else:
        theirs = jnp.zeros_like(pack)
    received = []
    if groups > 1:
        sends = messages(where, pack, theirs, groups, span)
        for k in sorted(range(1, groups), key=lambda k: k % 2 == 0):
            pairs = [
                (g * span + s, (g + k) % groups * span + s) for g in range(groups) for s in range(span)
            ]
            received.append((k, lax.ppermute(sends[k - 1], "frame", pairs)))
        received = [v for _, v in sorted(received, key=lambda kv: kv[0])]
        enter = entering(where, received, groups)
    else:
        enter = jnp.zeros((2, pack.shape[1] - LOGS, channels // span), BF16)
    other = lax.ppermute(enter, "frame", swap) if span == 2 else enter
    inner, gate = {}, {}
    for k in order:
        inner[k] = inside(k, xfs[k], xbs[k], fixed, bcs[k], cums[k], cum_ts[k], skip, heads)
        gate[k] = gates(pieces[k], w_gate)
    starts, fades = starts_of(where, xfs, xbs, fixed, b_ts, fading, lasts, spread, heads)

    def block(k):
        return finish(
            where,
            k,
            inner[k],
            bcs[k],
            reached[k],
            gate[k],
            starts,
            fades,
            theirs,
            enter,
            other,
            spread,
            gain,
            w_out,
        )

    up_a = up_b = down_a = down_b = None
    for hop in range(far, 0, -1):
        if 2 * hop == ring:
            a, b = block(hop)
            up_a, down_b = up(a), down(b)
            continue
        (above_a, above_b), (below_a, below_b) = block(hop), block(ring - hop)
        up_b = up(above_b if up_b is None else plus(above_b, up_b))
        down_a = down(below_a if down_a is None else plus(below_a, down_a))
        up_a = up(above_a if up_a is None else plus(above_a, up_a))
        down_b = down(below_b if down_b is None else plus(below_b, down_b))
    value, square = block(0)
    halves = [[v for v in pair if v is not None] for pair in ((up_a, down_a), (up_b, down_b))]
    return normalize(value, square, halves, channels * ring).reshape(tokens.shape)


def solution(mesh):
    return jax.shard_map(
        layer,
        mesh=mesh,
        in_specs=(
            P("frame", "row", None),
            P(None, "row"),
            P(None, "row"),
            P(),
            P(None, None, "row"),
            P(None, "row"),
            P(None, "row"),
            P(None, None, "row"),
            P(None, "row"),
            P("row"),
            P("row", None),
        ),
        out_specs=P("frame", "row", None),
        check_vma=False,
    )
```

```python
import math

import jax
import jax.numpy as jnp
from jax import lax
from jax.experimental import pallas as pl
from jax.experimental.pallas import tpu as pltpu
from jax.sharding import PartitionSpec as P


HEAD_DIM = 64
LANES = 128
LOGS = 8
FIRST = 1
SPLIT = 20_000_000_000
LOG2E = 1.0 / math.log(2.0)
F32 = jnp.float32
BF16 = jnp.bfloat16


def mib(size):
    return pltpu.CompilerParams(vmem_limit_bytes=size << 20)


def vmem():
    return pl.BlockSpec(memory_space=pltpu.VMEM)


def smem():
    return pl.BlockSpec(memory_space=pltpu.SMEM)


def dot(a, b):
    return jnp.dot(a, b, preferred_element_type=F32)


def silu(v):
    return v / (1.0 + jnp.exp(-v))


def two_parts(v, stride):
    high = v.astype(BF16).astype(F32)
    return (high + pltpu.roll(v - high, stride, 1)).astype(BF16)


def split(where, own, ring, edge):
    rows, depth = own.shape
    half = rows // 2

    def body(where, own, a, b, outer):
        a[...] = own[:half, :]
        b[...] = own[half:, :]

        @pl.when(where[0] == ring - 1)
        def _():
            outer[...] = own[rows - edge :, :]

        @pl.when(where[0] != ring - 1)
        def _():
            outer[...] = own[:edge, :]

    shapes = [(half, depth), (half, depth), (edge, depth)]
    return pl.pallas_call(
        body,
        in_specs=[smem(), vmem()],
        out_specs=[vmem()] * 3,
        out_shape=[jax.ShapeDtypeStruct(s, BF16) for s in shapes],
        compiler_params=mib(8),
        cost_estimate=pl.CostEstimate(flops=SPLIT, bytes_accessed=2 << 20, transcendentals=0),
        name="split",
    )(where, own)


def prepare(step_bias, decay_rate, skip_gain, channels):
    heads = step_bias.shape[1]
    rest = LANES - 2 * heads

    def body(bias, rate, skip, spread, rows, skips):
        lane = lax.broadcasted_iota(jnp.int32, (LANES, channels), 0)
        head = lax.shift_right_logical(
            lax.broadcasted_iota(jnp.int32, (LANES, channels), 1), HEAD_DIM.bit_length() - 1
        )
        for d in range(2):
            hit = (lane == head + d * heads) | (lane == head + (2 + d) * heads)
            spread[d] = jnp.where(hit, 1.0, 0.0).astype(BF16)
        zeros = jnp.zeros((1, rest), F32)
        for at, ref in enumerate((bias, rate)):
            rows[at : at + 1, :] = jnp.concatenate([ref[0:1, :], ref[1:2, :], zeros], axis=1)
        pieces = jnp.concatenate([skip[...], jnp.zeros((2, LANES - heads), F32)], axis=1)
        p1 = pieces.astype(BF16).astype(F32)
        p2 = (pieces - p1).astype(BF16).astype(F32)
        p3 = pieces - p1 - p2
        stack = jnp.concatenate([p1, p2, p3, jnp.zeros((10, LANES), F32)], axis=0).astype(BF16)
        wide = dot(stack, spread[0])
        skips[...] = wide[0:2] + wide[2:4] + wide[4:6]

    shapes = [((2, LANES, channels), BF16), ((2, LANES), F32), ((2, channels), F32)]
    return pl.pallas_call(
        body,
        in_specs=[vmem()] * 3,
        out_specs=[vmem()] * 3,
        out_shape=[jax.ShapeDtypeStruct(*s) for s in shapes],
        compiler_params=mib(8),
        name="prepare",
    )(step_bias, decay_rate, skip_gain)


def gather(refs, stacked):
    at = 0
    for ref in refs:
        stacked[at : at + ref.shape[0], :] = ref[...]
        at += ref.shape[0]


def conv_of(window, taps, backward, count):
    reach = taps.shape[0] - 1
    total = 0.0
    for j in range(reach + 1):
        start = reach - j if backward else j
        total = total + taps[j : j + 1] * window[start : start + count]
    return silu(total)


def block_states(pieces, bounds, where, w_value, w_state, w_step, taps, small_rows, heads):
    rows, depth = sum(p.shape[0] for p in pieces), pieces[0].shape[1]
    channels, states, steps = w_value.shape[1], w_state.shape[1], w_step.shape[0]
    size = states // 4
    reach = taps.shape[1] - 1
    count, around = len(pieces), len(bounds)
    pad = 8
    total = rows + (2 * pad if around else 0)

    def body(where, *refs):
        src, refs = refs[:count], refs[count:]
        edges, refs = refs[:around], refs[around:]
        wv, ws, wt, taps, small = refs[:5]
        xf, xb, ends, bc, b_t, cum_out, cum_t, reached, fade, last_out = refs[5:15]
        stacked, sx = refs[-2:]
        gather(src, stacked)
        for j, ref in enumerate(edges):

            @pl.when(lax.rem(where[0] + 1, around) == j)
            def _(ref=ref):
                stacked[rows : rows + pad, :] = ref[...]

            @pl.when(where[0] == j)
            def _(ref=ref):
                stacked[rows + pad :, :] = ref[...]

        sx[:pad, :] = jnp.zeros((pad, channels), F32)
        sx[pad + rows :, :] = jnp.zeros((pad, channels), F32)

        def conv(n):
            for at in range(n, n + 256, LANES):
                cols = slice(at, at + LANES)
                ahead, behind = taps[0, :, cols], taps[1, :, cols]
                for base in range(pad, pad + rows, 64):
                    views = {o: sx[base + o : base + o + 64, cols] for o in range(-reach, reach + 1)}
                    f = sum(ahead[j : j + 1] * views[j - reach] for j in range(reach + 1))
                    b = sum(behind[j : j + 1] * views[reach - j] for j in range(reach + 1))
                    xf[base - pad : base - pad + 64, cols] = silu(f).astype(BF16)
                    xb[base - pad : base - pad + 64, cols] = silu(b).astype(BF16)

        for n in range(0, channels, 256):
            cols = slice(n, n + 256)
            x = dot(stacked[...], wv[:, cols]).astype(BF16)
            sx[pad : pad + rows, cols] = x[:rows].astype(F32)
            ends[:pad, cols] = x[:pad]
            ends[pad : 2 * pad, cols] = x[rows - pad : rows]
            if around:
                ends[2 * pad :, cols] = x[rows:]
            if n:
                conv(n - 256)
        raw = lax.dot_general(
            stacked[:rows, :], wt[...], (((1,), (1,)), ((), ())), preferred_element_type=F32
        )
        raw = jnp.concatenate(
            [raw.astype(BF16).astype(F32), jnp.zeros((rows, LANES - steps), F32)], axis=1
        )
        for n in range(0, states, 256):
            bc[:, n : n + 256] = dot(stacked[:rows, :], ws[:, n : n + 256]).astype(BF16)
        conv(channels - 256)

        lane = lax.broadcasted_iota(jnp.int32, (rows, LANES), 1)
        used, forward = lane < 2 * heads, lane < heads
        low_row, low_col = (lax.broadcasted_iota(jnp.int32, (rows, rows), d) for d in (0, 1))
        both = jnp.concatenate(
            [
                jnp.where(low_row >= low_col, 1.0, 0.0).astype(BF16),
                jnp.where(low_row <= low_col, 1.0, 0.0).astype(BF16),
            ],
            axis=0,
        )
        v = raw + small[0:1, :]
        dt = jnp.maximum(v, 0.0) + jnp.log1p(jnp.exp(-jnp.abs(v)))
        dt = jnp.where(used, dt, 0.0)
        a = -dt * small[1:2, :] * LOG2E
        a1 = a.astype(BF16).astype(F32)
        a2 = (a - a1).astype(BF16).astype(F32)
        a3 = a - a1 - a2
        parts = a1 + pltpu.roll(a2, 2 * heads, 1) + pltpu.roll(a3, 4 * heads, 1)
        sums = dot(both, parts.astype(BF16))
        sums = pltpu.roll(sums, LANES - 4 * heads, 1) + pltpu.roll(sums, LANES - 2 * heads, 1) + sums
        cum = jnp.where(used, jnp.where(forward, sums[:rows], sums[rows:]), 0.0)
        last = jnp.where(forward[:1], cum[rows - 1 :], cum[:1])
        last_out[...] = jnp.broadcast_to(last, last_out.shape)
        cum_out[...] = cum
        cum_t[...] = (cum + pltpu.roll(dt, 2 * heads, 1)).T
        reached[...] = two_parts(jnp.where(used, jnp.exp2(cum), 0.0), 2 * heads)
        fade[...] = jnp.exp2(last - cum) * dt
        for d in range(2):
            b_t[d] = bc[:, d * 2 * size : (2 * d + 1) * size].astype(F32).T.astype(BF16)

    shapes = [
        ((rows, channels), BF16),
        ((rows, channels), BF16),
        ((4 * pad if around else 2 * pad, channels), BF16),
        ((rows, states), BF16),
        ((2, size, rows), BF16),
        ((rows, LANES), F32),
        ((LANES, rows), F32),
        ((rows, LANES), BF16),
        ((rows, LANES), F32),
        ((8, LANES), F32),
    ]
    width = channels + states + LANES
    return pl.pallas_call(
        body,
        in_specs=[smem()] + [vmem()] * (count + around + 5),
        out_specs=[vmem()] * len(shapes),
        out_shape=[jax.ShapeDtypeStruct(*s) for s in shapes],
        scratch_shapes=[
            pltpu.VMEM((total, depth), BF16),
            pltpu.VMEM((rows + 2 * pad, channels), F32),
        ],
        compiler_params=mib(16),
        cost_estimate=pl.CostEstimate(
            flops=3 * total * depth * width, bytes_accessed=2 * depth * width, transcendentals=0
        ),
        name="block_states",
    )(where, *pieces, *bounds, w_value, w_state, w_step, taps, small_rows)


def frame_logs(where, lasts, ring):
    at = [lax.rem(where[0] + k, ring) for k in range(ring)]
    rows = [ref[0:1, :] for ref in lasts]

    def between(low, high):
        out = jnp.zeros_like(rows[0])
        for place, row in zip(at, rows):
            out += jnp.where(jnp.logical_and(place > low, place < high), row, 0.0)
        return out

    return at, rows, between


def spread_rows(rows, heads, spread):
    lane = lax.broadcasted_iota(jnp.int32, rows[0].shape, 1)
    rows = [jnp.where(lane < 2 * heads, jnp.exp2(r), 0.0) for r in rows]
    short = -len(rows) % 8
    if short:
        rows.append(jnp.zeros((short, LANES), F32))
    packed = two_parts(jnp.concatenate(rows, axis=0), 2 * heads)
    return [dot(packed, spread[d]) for d in range(2)]


def early_sums(where, early, late, ring, blocks, bounded, taps, spread, heads):
    rows, channels = blocks[0][0].shape
    size = blocks[0][4].shape[1]
    pad = 8
    reach = taps.shape[1] - 1
    count = len(early)
    needed = [[blocks[k][i] for k in early] for i in (0, 1, 2, 4, 8)]

    def body(where, *refs):
        xf, xb, ends, b_t, fades = (dict(zip(early, refs[i * count : (i + 1) * count])) for i in range(5))
        taps, spread, fixed, added, qs = refs[5 * count :]
        row = lax.broadcasted_iota(jnp.int32, (rows, LANES), 0)
        forward = lax.broadcasted_iota(jnp.int32, (rows, LANES), 1) < heads
        fixed[...] = jnp.zeros_like(fixed)
        for i, k in enumerate(early):
            at = lax.rem(where[0] + k, ring)
            below, above = (k - 1) % ring, (k + 1) % ring
            fade = fades[k][...]
            if below == late:
                fade = jnp.where(forward & (row < pad), 0.0, fade)
            if above == late:
                fade = jnp.where(jnp.logical_not(forward) & (row >= rows - pad), 0.0, fade)
            qs[i * rows : (i + 1) * rows, :] = two_parts(fade, 2 * heads)
            for n in range(0, channels, 256):
                cols = slice(n, n + 256)
                own = ends[k][: 2 * pad, cols].astype(F32)
                if below != late:
                    outer = ends[bounded][2 * pad : 3 * pad, cols]
                    before = jnp.where(at == 0, outer, ends[below][pad : 2 * pad, cols]).astype(F32)
                    window = jnp.concatenate([before, own[:pad]], axis=0)
                    fixed[k, :pad, cols] = conv_of(
                        window[pad - reach :], taps[0, :, cols], False, pad
                    ).astype(BF16)
                if above != late:
                    outer = ends[bounded][3 * pad :, cols]
                    after = jnp.where(at == ring - 1, outer, ends[above][:pad, cols]).astype(F32)
                    window = jnp.concatenate([own[pad:], after], axis=0)
                    fixed[k, pad:, cols] = conv_of(
                        window[: pad + reach], taps[1, :, cols], True, pad
                    ).astype(BF16)
        for d in range(2):
            for n in range(0, channels, 256):
                cols = slice(n, n + 256)
                scale = dot(qs[...], spread[d, :, cols])
                for i, k in enumerate(early):
                    x = patched((xf, xb)[d][k], fixed, k, cols, pad, d)
                    part = slice(i * rows, (i + 1) * rows)
                    added[i, d, :, cols] = dot(b_t[k][d], (scale[part] * x.astype(F32)).astype(BF16))

    return pl.pallas_call(
        body,
        in_specs=[smem()] + [vmem()] * (5 * count + 2),
        out_specs=[vmem()] * 2,
        out_shape=[
            jax.ShapeDtypeStruct((ring, 2 * pad, channels), BF16),
            jax.ShapeDtypeStruct((count, 2, size, channels), F32),
        ],
        scratch_shapes=[pltpu.VMEM((count * rows, LANES), BF16)],
        compiler_params=mib(16),
        cost_estimate=pl.CostEstimate(flops=1_000_000_000, bytes_accessed=4 << 20, transcendentals=0),
        name="early_sums",
    )(where, *[v for group in needed for v in group], taps, spread)


def combine(where, early, late, ring, blocks, bounded, lasts, fixed, added, taps, spread, heads):
    rows, channels = blocks[0][0].shape
    size = blocks[0][4].shape[1]
    pad = 8
    reach = taps.shape[1] - 1
    below, above = (late - 1) % ring, (late + 1) % ring
    sides = {k: i for i, k in enumerate(dict.fromkeys((late, below, above, bounded)))}
    count = len(sides)
    needed = [blocks[k][i] for i in (2, 4, 8) for k in sides]

    def body(where, *refs):
        ends, b_t, fades = (
            {k: refs[i * count + j] for k, j in sides.items()} for i in range(3)
        )
        refs = refs[3 * count :]
        xf, xb, early_fixed, added = refs[:4]
        lasts = refs[4 : 4 + ring]
        taps, spread, pack, fixed, carried = refs[4 + ring :]
        at, logs, between = frame_logs(where, lasts, ring)
        forward = lax.broadcasted_iota(jnp.int32, logs[0].shape, 1) < heads
        later = [jnp.where(forward, between(p, ring), between(-1, p)) for p in at]
        fixed[...] = early_fixed[...]

        def mend(k, d):
            first, final = at[k] == 0, at[k] == ring - 1
            for n in range(0, channels, 256):
                cols = slice(n, n + 256)
                own = ends[k][: 2 * pad, cols].astype(F32)
                if d == 0:
                    outer = ends[bounded][2 * pad : 3 * pad, cols]
                    next_to = ends[(k - 1) % ring][pad : 2 * pad, cols]
                    before = jnp.where(first, outer, next_to).astype(F32)
                    window = jnp.concatenate([before, own[:pad]], axis=0)[pad - reach :]
                    fixed[k, :pad, cols] = conv_of(window, taps[0, :, cols], False, pad).astype(BF16)
                else:
                    outer = ends[bounded][3 * pad :, cols]
                    next_to = ends[(k + 1) % ring][:pad, cols]
                    after = jnp.where(final, outer, next_to).astype(F32)
                    window = jnp.concatenate([own[pad:], after], axis=0)[: pad + reach]
                    fixed[k, pad:, cols] = conv_of(window, taps[1, :, cols], True, pad).astype(BF16)

        for k, d in ((late, 0), (late, 1), (above, 0), (below, 1)):
            mend(k, d)
        q = two_parts(fades[late][...] * jnp.exp2(later[late]), 2 * heads)
        q_above = two_parts(fades[above][:pad, :] * jnp.exp2(later[above]), 2 * heads)
        q_below = two_parts(fades[below][rows - pad :, :] * jnp.exp2(later[below]), 2 * heads)
        weights = spread_rows([later[k] for k in early], heads, spread)
        total = sum(logs[1:], logs[0])
        l1 = total.astype(BF16).astype(F32)
        l2 = (total - l1).astype(BF16).astype(F32)
        three = jnp.concatenate([l1, l2, total - l1 - l2, jnp.zeros((LOGS - 3, LANES), F32)], axis=0)
        carried[...] = jnp.zeros_like(carried)
        for d in range(2):
            pack[d, size:, :] = dot(three.astype(BF16), spread[d]).astype(BF16)
            side = above if d == 0 else below
            place = slice(rows, rows + pad) if d == 0 else slice(2 * rows - pad, 2 * rows)
            b_all = jnp.concatenate([b_t[late][d], b_t[side][d]], axis=1)
            for n in range(0, channels, 256):
                cols = slice(n, n + 256)
                x = patched((xf, xb)[d], fixed, late, cols, pad, d)
                scale = dot(q, spread[d, :, cols])
                carried[d, :rows, :] = (scale * x.astype(F32)).astype(BF16)
                scale = dot(q_above if d == 0 else q_below, spread[d, :, cols])
                x = fixed[side, :pad, cols] if d == 0 else fixed[side, pad:, cols]
                carried[d, place, :] = (scale * x.astype(F32)).astype(BF16)
                state = dot(b_all, carried[d])
                for i in range(len(early)):
                    state += weights[d][i : i + 1, cols] * added[i, d, :, cols]
                pack[d, :size, cols] = state.astype(BF16)

    return pl.pallas_call(
        body,
        in_specs=[smem()] + [vmem()] * (3 * count + 6 + ring),
        out_specs=[vmem()] * 2,
        out_shape=[
            jax.ShapeDtypeStruct((2, size + LOGS, channels), BF16),
            jax.ShapeDtypeStruct((ring, 2 * pad, channels), BF16),
        ],
        scratch_shapes=[pltpu.VMEM((2, 2 * rows, 256), BF16)],
        compiler_params=mib(16),
        cost_estimate=pl.CostEstimate(flops=500_000_000, bytes_accessed=4 << 20, transcendentals=0),
        name="combine",
    )(where, *needed, blocks[late][0], blocks[late][1], fixed, added, *lasts, taps, spread)


def patched(x, fixed, k, cols, pad, d):
    rows = x.shape[0]
    if d == 0:
        return jnp.concatenate([fixed[k, :pad, cols], x[pad:, cols]], axis=0)
    return jnp.concatenate([x[: rows - pad, cols], fixed[k, pad:, cols]], axis=0)


def starts_of(where, xfs, xbs, fixed, b_ts, fades, lasts, spread, heads):
    ring = len(xfs)
    rows, channels = xfs[0].shape
    size = b_ts[0].shape[1]
    pad = fixed.shape[1] // 2

    def body(where, *refs):
        xf, xb, b_t, fades, lasts = (refs[i * ring : (i + 1) * ring] for i in range(5))
        fixed, spread, starts, fades_out, qs = refs[5 * ring :]
        at, logs, between = frame_logs(where, lasts, ring)
        forward = lax.broadcasted_iota(jnp.int32, logs[0].shape, 1) < heads
        fade = spread_rows(
            [jnp.where(forward, between(-1, p), between(p, ring)) for p in at], heads, spread
        )
        for d in range(2):
            fades_out[d] = fade[d]
        for k in range(ring):
            qs[k * rows : (k + 1) * rows, :] = two_parts(fades[k][...], 2 * heads)
        weights = [
            spread_rows(
                [
                    jnp.where(forward, between(at[k], at[j]), between(at[j], at[k]))
                    for k in range(ring)
                ],
                heads,
                spread,
            )
            for j in range(ring)
        ]
        for d in range(2):
            for n in range(0, channels, 256):
                cols = slice(n, n + 256)
                scale = dot(qs[...], spread[d, :, cols])
                for k in range(ring):
                    x = patched((xf, xb)[d][k], fixed, k, cols, pad, d)
                    part = slice(k * rows, (k + 1) * rows)
                    added = dot(b_t[k][d], (scale[part] * x.astype(F32)).astype(BF16))
                    for j in range(ring):
                        if j == k:
                            continue
                        before = at[k] < at[j] if d == 0 else at[k] > at[j]
                        term = jnp.where(before, weights[j][d][k : k + 1, cols], 0.0) * added
                        if k == (1 if j == 0 else 0):
                            starts[j, d, :, cols] = term
                        else:
                            starts[j, d, :, cols] += term

    return pl.pallas_call(
        body,
        in_specs=[smem()] + [vmem()] * (5 * ring + 2),
        out_specs=[vmem()] * 2,
        out_shape=[
            jax.ShapeDtypeStruct((ring, 2, size, channels), F32),
            jax.ShapeDtypeStruct((2, ring + -ring % 8, channels), F32),
        ],
        scratch_shapes=[pltpu.VMEM((ring * rows, LANES), BF16)],
        compiler_params=mib(16),
        cost_estimate=pl.CostEstimate(flops=1_200_000_000, bytes_accessed=8 << 20, transcendentals=0),
        name="starts",
    )(where, *xfs, *xbs, *b_ts, *fades, *lasts, fixed, spread)


def inside(k, xf, xb, fixed, bc, cum, cum_t, skip, heads):
    rows, channels = xf.shape
    size = bc.shape[1] // 4

    pad = fixed.shape[1] // 2

    def body(xf, xb, fixed, bc, cum, cum_t, skip, y):
        row, col = (lax.broadcasted_iota(jnp.int32, (rows, rows), d) for d in (0, 1))
        first = lax.broadcasted_iota(jnp.int32, (rows, LANES), 1) < HEAD_DIM
        scores = []
        for d in range(2):
            b_rows = bc[:, 2 * d * size : (2 * d + 1) * size]
            c_rows = bc[:, (2 * d + 1) * size : (2 * d + 2) * size]
            s = lax.dot_general(
                c_rows, b_rows, (((1,), (1,)), ((), ())), preferred_element_type=F32
            )
            scores.append(jnp.where(row >= col if d == 0 else row <= col, s, 0.0))
        for pair in range(channels // LANES):
            cols = slice(pair * LANES, (pair + 1) * LANES)
            weights = []
            for h in range(pair * (LANES // HEAD_DIM), (pair + 1) * (LANES // HEAD_DIM)):
                sides = []
                for d in range(2):
                    at = d * heads + h
                    gap = jnp.minimum(cum[:, at : at + 1] - cum_t[at : at + 1, :], 0.0)
                    dt = cum_t[2 * heads + at : 2 * heads + at + 1, :]
                    sides.append((jnp.exp2(gap) * (scores[d] * dt)).astype(BF16))
                weights.append(jnp.concatenate(sides, axis=1))
            sides = [patched(x, fixed, k, cols, pad, d) for d, x in enumerate((xf, xb))]
            x_pair = jnp.concatenate(sides, axis=0)
            out = dot(jnp.concatenate(weights, axis=0), x_pair)
            total = jnp.where(first, out[:rows], out[rows:])
            total += skip[0:1, cols] * sides[0].astype(F32)
            total += skip[1:2, cols] * sides[1].astype(F32)
            y[:, cols] = total

    return pl.pallas_call(
        body,
        in_specs=[vmem()] * 7,
        out_specs=vmem(),
        out_shape=jax.ShapeDtypeStruct((rows, channels), F32),
        compiler_params=mib(12),
        cost_estimate=pl.CostEstimate(flops=1_200_000_000, bytes_accessed=2 << 20, transcendentals=0),
        name="inside",
    )(xf, xb, fixed, bc, cum, cum_t, skip)


def gates(pieces, w_gate):
    rows, depth = sum(p.shape[0] for p in pieces), pieces[0].shape[1]
    channels, count = w_gate.shape[1], len(pieces)

    def body(*refs):
        wg, gate, block = refs[count:]
        gather(refs[:count], block)
        for n in range(0, channels, 256):
            raw = dot(block[...], wg[:, n : n + 256]).astype(BF16)
            gate[:, n : n + 256] = silu(raw.astype(F32))

    return pl.pallas_call(
        body,
        in_specs=[vmem()] * (count + 1),
        out_specs=vmem(),
        out_shape=jax.ShapeDtypeStruct((rows, channels), F32),
        scratch_shapes=[pltpu.VMEM((rows, depth), BF16)],
        compiler_params=mib(12),
        cost_estimate=pl.CostEstimate(
            flops=2 * rows * depth * channels, bytes_accessed=2 * depth * channels, transcendentals=0
        ),
        name="gates",
    )(*pieces, w_gate)


def log_rows(rows):
    rows = rows.astype(F32)
    return rows[0:1] + rows[1:2] + rows[2:3]


def messages(where, mine, theirs, groups, parts):
    size, channels = mine.shape[1] - LOGS, mine.shape[2]
    width = channels // parts

    def body(where, mine, theirs, *outs):
        group, second = where[1], where[2] == 1
        cols = pl.ds(pl.multiple_of(where[2] * width, LANES), width)
        for d in range(2):
            own, other = log_rows(mine[d, size:, cols]), log_rows(theirs[d, size:, cols])
            later = second if d == 0 else jnp.logical_not(second)
            scale_own = jnp.where(later, 1.0, jnp.exp2(other))
            scale_other = jnp.where(later, jnp.exp2(own), 1.0)
            total = own + other
            l1 = total.astype(BF16).astype(F32)
            l2 = (total - l1).astype(BF16).astype(F32)
            logs = jnp.concatenate(
                [l1, l2, total - l1 - l2, jnp.zeros((LOGS - 3, width), F32)], axis=0
            ).astype(BF16)
            state = scale_own * mine[d, :size, cols].astype(F32)
            state = (state + scale_other * theirs[d, :size, cols].astype(F32)).astype(BF16)
            for k, out in enumerate(outs, 1):
                onward = group + k < groups

                @pl.when(onward if d == 0 else jnp.logical_not(onward))
                def _(out=out):
                    out[:size, :] = state
                    out[size:, :] = logs

    return pl.pallas_call(
        body,
        in_specs=[smem(), vmem(), vmem()],
        out_specs=[vmem()] * (groups - 1),
        out_shape=[jax.ShapeDtypeStruct((size + LOGS, width), BF16)] * (groups - 1),
        compiler_params=mib(16),
        cost_estimate=pl.CostEstimate(flops=1_000_000, bytes_accessed=2 << 20, transcendentals=0),
        name="messages",
    )(where, mine, theirs)


def entering(where, received, groups):
    size, width = received[0].shape[0] - LOGS, received[0].shape[1]

    def body(where, *refs):
        got, out = refs[:-1], refs[-1]
        group = where[1]
        for d in range(2):
            log = jnp.zeros((1, width), F32)
            state = jnp.zeros((size, width), F32)
            for far in range(1, groups):
                ref = got[far - 1] if d == 0 else got[groups - far - 1]
                holds = far <= (group if d == 0 else groups - 1 - group)
                scale = jnp.where(holds, jnp.exp2(log), 0.0)
                state += scale * ref[:size, :].astype(F32)
                log = jnp.where(holds, log + log_rows(ref[size:, :]), log)
            out[d] = state.astype(BF16)

    return pl.pallas_call(
        body,
        in_specs=[smem()] + [vmem()] * len(received),
        out_specs=vmem(),
        out_shape=jax.ShapeDtypeStruct((2, size, width), BF16),
        compiler_params=mib(16),
        cost_estimate=pl.CostEstimate(flops=1_000_000, bytes_accessed=2 << 20, transcendentals=0),
        name="entering",
    )(where, *received)


SUB = 16


def pack_squares(row):
    high = row.astype(BF16).astype(F32)
    return jnp.concatenate([high, row - high, jnp.zeros((SUB - 2, LANES), F32)], axis=0).astype(BF16)


def squares_of(packed):
    v = packed.astype(F32)
    return v[0:1] + v[1:2]


def finish(where, k, y, bc, reached, gate, starts, fades, theirs, mine, other, spread, gain, w_out):
    rows, channels = y.shape
    size = bc.shape[1] // 4
    width = w_out.shape[1]
    half = rows // 2
    last = k == 0
    part = mine.shape[2]
    step = min(256, part)
    across = width // LANES
    count = half // SUB * across

    def body(where, y, bc, reached, gate, starts, fades, theirs, mine, other, spread, gain, w_out, *refs):
        outs, scaled = refs[:-1], refs[-1]
        second = where[2] == 1
        square = jnp.zeros((rows, LANES), F32)
        for n in range(0, channels, step):
            cols = slice(n, n + step)
            total = y[:, cols]
            for d in range(2):
                c_rows = bc[:, (2 * d + 1) * size : (2 * d + 2) * size]
                near = second if d == 0 else jnp.logical_not(second)
                at = slice(n % part, n % part + step)
                enter = jnp.where(where[2] == n // part, mine[d, :, at], other[d, :, at]).astype(F32)
                log = jnp.where(near, log_rows(theirs[d, size:, cols]), 0.0)
                enter = jnp.exp2(log) * enter
                enter += jnp.where(near, theirs[d, :size, cols].astype(F32), 0.0)
                state = starts[0, d, :, cols] + fades[d, k : k + 1, cols] * enter
                total += dot(reached[...], spread[d, :, cols]) * dot(c_rows, state.astype(BF16))
            gated = total * gate[:, cols]
            for t in range(0, step, LANES):
                square += gated[:, t : t + LANES] * gated[:, t : t + LANES]
            scaled[:, cols] = (gated * gain[:, cols]).astype(BF16)
        sums = jnp.broadcast_to(jnp.sum(square, axis=1, keepdims=True), (rows, LANES))
        row = sums.T[0:1, :]
        if last:
            outs[1][...] = jnp.broadcast_to(row, (SUB, rows))
        else:
            for out in outs:
                out[count] = pack_squares(row)
        for n in range(0, width, 256):
            value = dot(scaled[...], w_out[:, n : n + 256])
            if last:
                outs[0][:, n : n + 256] = value
                continue
            value = value.astype(BF16)
            for i in range(rows // SUB):
                for j in range(0, 256, LANES):
                    tile = value[i * SUB : (i + 1) * SUB, j : j + LANES]
                    place = i % (half // SUB) * across + (n + j) // LANES
                    outs[i * SUB // half][place] = tile

    if last:
        shapes = [((rows, width), F32), ((SUB, rows), F32)]
    else:
        shapes = [((count + 1, SUB, LANES), BF16)] * 2
    specs = [smem()] + [vmem()] * 12
    specs[5] = pl.BlockSpec((1,) + starts.shape[1:], lambda i: (k, 0, 0, 0))
    return pl.pallas_call(
        body,
        grid=(1,),
        in_specs=specs,
        out_specs=[vmem()] * len(shapes),
        out_shape=[jax.ShapeDtypeStruct(*s) for s in shapes],
        scratch_shapes=[pltpu.VMEM((rows, channels), BF16)],
        compiler_params=mib(16),
        cost_estimate=pl.CostEstimate(
            flops=2 * rows * channels * width, bytes_accessed=2 * channels * width, transcendentals=0
        ),
        name="finish",
    )(where, y, bc, reached, gate, starts, fades, theirs, mine, other, spread, gain, w_out)


def plus(value, got):
    count = value.shape[0] - 1

    def body(value, got, out):
        for n in range(0, count, 8):
            part = slice(n, min(n + 8, count))
            out[part] = (value[part].astype(F32) + got[part].astype(F32)).astype(BF16)
        out[count] = pack_squares(squares_of(value[count]) + squares_of(got[count]))

    return pl.pallas_call(
        body,
        in_specs=[vmem()] * 2,
        out_specs=vmem(),
        out_shape=jax.ShapeDtypeStruct(value.shape, BF16),
        compiler_params=mib(8),
        name="plus",
    )(value, got)


def normalize(part, into, value, square, got, channels):
    rows, width = value.shape
    half = rows // 2
    across = width // LANES
    count = half // SUB * across
    held = [] if into is None else [into]

    def body(value, square, *refs):
        ins, out = refs[: len(got)], refs[-1]
        sums = square[0:1, :]
        for ref in ins:
            sums = sums + squares_of(ref[count])
        scale = lax.rsqrt(sums / channels + 1e-05)
        scale = jnp.broadcast_to(scale, (LANES, rows)).T[part * half : (part + 1) * half]
        for i in range(half // SUB):
            for j in range(across):
                at = (slice(i * SUB, (i + 1) * SUB), slice(j * LANES, (j + 1) * LANES))
                total = value[at]
                for ref in ins:
                    total = total + ref[i * across + j].astype(F32)
                out[at] = (total * scale[at[0], :]).astype(BF16)

    block = pl.BlockSpec((half, width), lambda n: (part, 0))
    return pl.pallas_call(
        body,
        grid=(1,),
        in_specs=[block] + [vmem()] * (1 + len(got)) + [pl.BlockSpec(memory_space=pl.ANY)] * len(held),
        out_specs=block,
        out_shape=jax.ShapeDtypeStruct(value.shape, BF16),
        input_output_aliases={2 + len(got): 0} if held else {},
        compiler_params=mib(8),
        name="normalize",
    )(value, square, *got, *held)


def ring_pairs(count, step):
    return [(i, (i + step) % count) for i in range(count)]


def layer(
    tokens,
    w_gate,
    w_value,
    w_state_proj,
    w_step,
    step_bias,
    decay_rate,
    conv_taps,
    skip_gain,
    norm_gain,
    w_out,
):
    ring, frames = lax.axis_size("row"), lax.axis_size("frame")
    row, frame = lax.axis_index("row"), lax.axis_index("frame")
    channels, heads = w_gate.shape[1], step_bias.shape[1]
    span = 2 if frames % 2 == 0 else 1
    groups = frames // span
    where = jnp.stack([row, frame // span, frame % span]).astype(jnp.int32)
    own = tokens.reshape(-1, tokens.shape[2])
    far = ring // 2
    edge = 8
    end = ring - 1

    def up(v):
        return lax.ppermute(v, "row", ring_pairs(ring, 1))

    def down(v):
        return lax.ppermute(v, "row", ring_pairs(ring, -1))

    first, second, outer = split(where, own, ring, edge)
    pieces = {0: [first, second]}
    order = [0]
    from_below, from_above = [first, second], [second, first]
    for hop in range(1, far + 1):
        a, c = up(from_below[0]), down(from_above[0])
        if 2 * hop == ring:
            pieces[hop] = [a, c]
            order.append(hop)
        else:
            b, d = up(from_below[1]), down(from_above[1])
            from_below, from_above = [a, b], [c, d]
            pieces[ring - hop], pieces[hop] = [a, b], [d, c]
            order += [ring - hop, hop]
    bounds = []
    for j in range(ring):
        pairs = [(f * ring + end, (f + 1) * ring + (end + j) % ring) for f in range(frames - 1)]
        pairs += [((f + 1) * ring, f * ring + j) for f in range(frames - 1)]
        bounds.append(lax.ppermute(outer, ("frame", "row"), pairs))

    steps = jnp.swapaxes(w_step, 1, 2).reshape(-1, w_step.shape[1])
    spread, small_rows, skip = prepare(step_bias, decay_rate, skip_gain, channels)
    gain = norm_gain.reshape(1, -1)

    blocks = {}
    bounded = order[-2]
    for k in order:
        blocks[k] = block_states(
            pieces[k],
            bounds if k == bounded else [],
            where,
            w_value,
            w_state_proj,
            steps,
            conv_taps,
            small_rows,
            heads,
        )
    xfs, xbs, _, bcs, b_ts, cums, cum_ts, reached, fading, lasts = (
        [blocks[k][i] for k in range(ring)] for i in range(len(blocks[0]))
    )
    early, late = order[:-1], order[-1]
    shared = (early, late, ring, blocks, bounded)
    fixed, added = early_sums(where, *shared, conv_taps, spread, heads)
    pack, fixed = combine(where, *shared, lasts, fixed, added, conv_taps, spread, heads)

    if span == 2:
        swap = [(i, i ^ 1) for i in range(frames)]
        theirs = lax.ppermute(pack, "frame", swap)
    else:
        theirs = jnp.zeros_like(pack)
    received = []
    if groups > 1:
        sends = messages(where, pack, theirs, groups, span)
        for k in sorted(range(1, groups), key=lambda k: k % 2 == 0):
            pairs = [
                (g * span + s, (g + k) % groups * span + s) for g in range(groups) for s in range(span)
            ]
            received.append((k, lax.ppermute(sends[k - 1], "frame", pairs)))
        received = [v for _, v in sorted(received, key=lambda kv: kv[0])]
        enter = entering(where, received, groups)
    else:
        enter = jnp.zeros((2, pack.shape[1] - LOGS, channels // span), BF16)
    other = lax.ppermute(enter, "frame", swap) if span == 2 else enter
    inner, gate = {}, {}
    for k in order:
        inner[k] = inside(k, xfs[k], xbs[k], fixed, bcs[k], cums[k], cum_ts[k], skip, heads)
        gate[k] = gates(pieces[k], w_gate)
    starts, fades = starts_of(where, xfs, xbs, fixed, b_ts, fading, lasts, spread, heads)

    def block(k):
        return finish(
            where,
            k,
            inner[k],
            bcs[k],
            reached[k],
            gate[k],
            starts,
            fades,
            theirs,
            enter,
            other,
            spread,
            gain,
            w_out,
        )

    up_a = up_b = down_a = down_b = None
    for hop in range(far, 0, -1):
        if 2 * hop == ring:
            a, b = block(hop)
            up_a, down_b = up(a), down(b)
            continue
        (above_a, above_b), (below_a, below_b) = block(hop), block(ring - hop)
        up_b = up(above_b if up_b is None else plus(above_b, up_b))
        down_a = down(below_a if down_a is None else plus(below_a, down_a))
        up_a = up(above_a if up_a is None else plus(above_a, up_a))
        down_b = down(below_b if down_b is None else plus(below_b, down_b))
    value, square = block(0)
    halves = [[v for v in pair if v is not None] for pair in ((up_a, down_a), (up_b, down_b))]
    mixed = normalize(FIRST, None, value, square, halves[FIRST], channels * ring)
    mixed = normalize(1 - FIRST, mixed, value, square, halves[1 - FIRST], channels * ring)
    return mixed.reshape(tokens.shape)


def solution(mesh):
    return jax.shard_map(
        layer,
        mesh=mesh,
        in_specs=(
            P("frame", "row", None),
            P(None, "row"),
            P(None, "row"),
            P(),
            P(None, None, "row"),
            P(None, "row"),
            P(None, "row"),
            P(None, None, "row"),
            P(None, "row"),
            P("row"),
            P("row", None),
        ),
        out_specs=P("frame", "row", None),
        check_vma=False,
    )
```

```python
import math

import jax
import jax.numpy as jnp
from jax import lax
from jax.experimental import pallas as pl
from jax.experimental.pallas import tpu as pltpu
from jax.sharding import PartitionSpec as P


HEAD_DIM = 64
LANES = 128
LOGS = 8
FIRST = 1
SPLIT = 20_000_000_000
LOG2E = 1.0 / math.log(2.0)
F32 = jnp.float32
BF16 = jnp.bfloat16


def mib(size):
    return pltpu.CompilerParams(vmem_limit_bytes=size << 20)


def vmem():
    return pl.BlockSpec(memory_space=pltpu.VMEM)


def smem():
    return pl.BlockSpec(memory_space=pltpu.SMEM)


def dot(a, b):
    return jnp.dot(a, b, preferred_element_type=F32)


def silu(v):
    return v / (1.0 + jnp.exp(-v))


def two_parts(v, stride):
    high = v.astype(BF16).astype(F32)
    return (high + pltpu.roll(v - high, stride, 1)).astype(BF16)


def split(where, own, ring, edge):
    rows, depth = own.shape
    half = rows // 2

    def body(where, own, a, b, outer):
        a[...] = own[:half, :]
        b[...] = own[half:, :]

        @pl.when(where[0] == ring - 1)
        def _():
            outer[...] = own[rows - edge :, :]

        @pl.when(where[0] != ring - 1)
        def _():
            outer[...] = own[:edge, :]

    shapes = [(half, depth), (half, depth), (edge, depth)]
    return pl.pallas_call(
        body,
        in_specs=[smem(), vmem()],
        out_specs=[vmem()] * 3,
        out_shape=[jax.ShapeDtypeStruct(s, BF16) for s in shapes],
        compiler_params=mib(8),
        cost_estimate=pl.CostEstimate(flops=SPLIT, bytes_accessed=2 << 20, transcendentals=0),
        name="split",
    )(where, own)


def prepare(step_bias, decay_rate, skip_gain, channels):
    heads = step_bias.shape[1]
    rest = LANES - 2 * heads

    def body(bias, rate, skip, spread, rows, skips):
        lane = lax.broadcasted_iota(jnp.int32, (LANES, channels), 0)
        head = lax.shift_right_logical(
            lax.broadcasted_iota(jnp.int32, (LANES, channels), 1), HEAD_DIM.bit_length() - 1
        )
        for d in range(2):
            hit = (lane == head + d * heads) | (lane == head + (2 + d) * heads)
            spread[d] = jnp.where(hit, 1.0, 0.0).astype(BF16)
        zeros = jnp.zeros((1, rest), F32)
        for at, ref in enumerate((bias, rate)):
            rows[at : at + 1, :] = jnp.concatenate([ref[0:1, :], ref[1:2, :], zeros], axis=1)
        pieces = jnp.concatenate([skip[...], jnp.zeros((2, LANES - heads), F32)], axis=1)
        p1 = pieces.astype(BF16).astype(F32)
        p2 = (pieces - p1).astype(BF16).astype(F32)
        p3 = pieces - p1 - p2
        stack = jnp.concatenate([p1, p2, p3, jnp.zeros((10, LANES), F32)], axis=0).astype(BF16)
        wide = dot(stack, spread[0])
        skips[...] = wide[0:2] + wide[2:4] + wide[4:6]

    shapes = [((2, LANES, channels), BF16), ((2, LANES), F32), ((2, channels), F32)]
    return pl.pallas_call(
        body,
        in_specs=[vmem()] * 3,
        out_specs=[vmem()] * 3,
        out_shape=[jax.ShapeDtypeStruct(*s) for s in shapes],
        compiler_params=mib(8),
        name="prepare",
    )(step_bias, decay_rate, skip_gain)


def gather(refs, stacked):
    at = 0
    for ref in refs:
        stacked[at : at + ref.shape[0], :] = ref[...]
        at += ref.shape[0]


def conv_of(window, taps, backward, count):
    reach = taps.shape[0] - 1
    total = 0.0
    for j in range(reach + 1):
        start = reach - j if backward else j
        total = total + taps[j : j + 1] * window[start : start + count]
    return silu(total)


def block_states(pieces, bounds, where, w_value, w_state, w_step, taps, small_rows, heads, brief):
    rows, depth = sum(p.shape[0] for p in pieces), pieces[0].shape[1]
    channels, states, steps = w_value.shape[1], w_state.shape[1], w_step.shape[0]
    size = states // 4
    reach = taps.shape[1] - 1
    count, around = len(pieces), len(bounds)
    pad = 8
    total = rows + (2 * pad if around else 0)

    def body(where, *refs):
        src, refs = refs[:count], refs[count:]
        edges, refs = refs[:around], refs[around:]
        wv, ws, wt, taps, small = refs[:5]
        xf, xb, ends, bc, b_t, cum_out, cum_t, reached, fade, last_out = refs[5:15]
        stacked, sx = refs[-2:]
        gather(src, stacked)
        for j, ref in enumerate(edges):

            @pl.when(lax.rem(where[0] + 1, around) == j)
            def _(ref=ref):
                stacked[rows : rows + pad, :] = ref[...]

            @pl.when(where[0] == j)
            def _(ref=ref):
                stacked[rows + pad :, :] = ref[...]

        sx[:pad, :] = jnp.zeros((pad, channels), F32)
        sx[pad + rows :, :] = jnp.zeros((pad, channels), F32)

        def conv(n):
            for at in range(n, n + 256, LANES):
                cols = slice(at, at + LANES)
                ahead, behind = taps[0, :, cols], taps[1, :, cols]
                for base in range(pad, pad + rows, 64):
                    views = {o: sx[base + o : base + o + 64, cols] for o in range(-reach, reach + 1)}
                    f = sum(ahead[j : j + 1] * views[j - reach] for j in range(reach + 1))
                    b = sum(behind[j : j + 1] * views[reach - j] for j in range(reach + 1))
                    xf[base - pad : base - pad + 64, cols] = silu(f).astype(BF16)
                    xb[base - pad : base - pad + 64, cols] = silu(b).astype(BF16)

        for n in range(0, channels, 256):
            cols = slice(n, n + 256)
            x = dot(stacked[...], wv[:, cols]).astype(BF16)
            sx[pad : pad + rows, cols] = x[:rows].astype(F32)
            ends[:pad, cols] = x[:pad]
            ends[pad : 2 * pad, cols] = x[rows - pad : rows]
            if around:
                ends[2 * pad :, cols] = x[rows:]
            if n:
                conv(n - 256)
        raw = lax.dot_general(
            stacked[:rows, :], wt[...], (((1,), (1,)), ((), ())), preferred_element_type=F32
        )
        raw = jnp.concatenate(
            [raw.astype(BF16).astype(F32), jnp.zeros((rows, LANES - steps), F32)], axis=1
        )
        wide = 2 * size
        for n in range(0, states, wide):
            cols = slice(n, n + (size if brief else wide))
            bc[:, cols] = dot(stacked[:rows, :], ws[:, cols]).astype(BF16)
        conv(channels - 256)

        lane = lax.broadcasted_iota(jnp.int32, (rows, LANES), 1)
        used, forward = lane < 2 * heads, lane < heads
        low_row, low_col = (lax.broadcasted_iota(jnp.int32, (rows, rows), d) for d in (0, 1))
        both = jnp.concatenate(
            [
                jnp.where(low_row >= low_col, 1.0, 0.0).astype(BF16),
                jnp.where(low_row <= low_col, 1.0, 0.0).astype(BF16),
            ],
            axis=0,
        )
        v = raw + small[0:1, :]
        dt = jnp.maximum(v, 0.0) + jnp.log1p(jnp.exp(-jnp.abs(v)))
        dt = jnp.where(used, dt, 0.0)
        a = -dt * small[1:2, :] * LOG2E
        a1 = a.astype(BF16).astype(F32)
        a2 = (a - a1).astype(BF16).astype(F32)
        a3 = a - a1 - a2
        parts = a1 + pltpu.roll(a2, 2 * heads, 1) + pltpu.roll(a3, 4 * heads, 1)
        sums = dot(both, parts.astype(BF16))
        sums = pltpu.roll(sums, LANES - 4 * heads, 1) + pltpu.roll(sums, LANES - 2 * heads, 1) + sums
        cum = jnp.where(used, jnp.where(forward, sums[:rows], sums[rows:]), 0.0)
        last = jnp.where(forward[:1], cum[rows - 1 :], cum[:1])
        last_out[...] = jnp.broadcast_to(last, last_out.shape)
        cum_out[...] = cum
        cum_t[...] = (cum + pltpu.roll(dt, 2 * heads, 1)).T
        reached[...] = two_parts(jnp.where(used, jnp.exp2(cum), 0.0), 2 * heads)
        fade[...] = jnp.exp2(last - cum) * dt
        for d in range(2):
            b_t[d] = bc[:, d * 2 * size : (2 * d + 1) * size].astype(F32).T.astype(BF16)

    shapes = [
        ((rows, channels), BF16),
        ((rows, channels), BF16),
        ((4 * pad if around else 2 * pad, channels), BF16),
        ((rows, states), BF16),
        ((2, size, rows), BF16),
        ((rows, LANES), F32),
        ((LANES, rows), F32),
        ((rows, LANES), BF16),
        ((rows, LANES), F32),
        ((8, LANES), F32),
    ]
    width = channels + states + LANES
    return pl.pallas_call(
        body,
        in_specs=[smem()] + [vmem()] * (count + around + 5),
        out_specs=[vmem()] * len(shapes),
        out_shape=[jax.ShapeDtypeStruct(*s) for s in shapes],
        scratch_shapes=[
            pltpu.VMEM((total, depth), BF16),
            pltpu.VMEM((rows + 2 * pad, channels), F32),
        ],
        compiler_params=mib(16),
        cost_estimate=pl.CostEstimate(
            flops=3 * total * depth * width, bytes_accessed=2 * depth * width, transcendentals=0
        ),
        name="block_states",
    )(where, *pieces, *bounds, w_value, w_state, w_step, taps, small_rows)


def frame_logs(where, lasts, ring):
    at = [lax.rem(where[0] + k, ring) for k in range(ring)]
    rows = [ref[0:1, :] for ref in lasts]

    def between(low, high):
        out = jnp.zeros_like(rows[0])
        for place, row in zip(at, rows):
            out += jnp.where(jnp.logical_and(place > low, place < high), row, 0.0)
        return out

    return at, rows, between


def spread_rows(rows, heads, spread):
    lane = lax.broadcasted_iota(jnp.int32, rows[0].shape, 1)
    rows = [jnp.where(lane < 2 * heads, jnp.exp2(r), 0.0) for r in rows]
    short = -len(rows) % 8
    if short:
        rows.append(jnp.zeros((short, LANES), F32))
    packed = two_parts(jnp.concatenate(rows, axis=0), 2 * heads)
    return [dot(packed, spread[d]) for d in range(2)]


def early_sums(where, early, late, ring, blocks, bounded, taps, spread, heads):
    rows, channels = blocks[0][0].shape
    size = blocks[0][4].shape[1]
    pad = 8
    reach = taps.shape[1] - 1
    count = len(early)
    needed = [[blocks[k][i] for k in early] for i in (0, 1, 2, 4, 8)]

    def body(where, *refs):
        xf, xb, ends, b_t, fades = (dict(zip(early, refs[i * count : (i + 1) * count])) for i in range(5))
        taps, spread, fixed, added, qs = refs[5 * count :]
        row = lax.broadcasted_iota(jnp.int32, (rows, LANES), 0)
        forward = lax.broadcasted_iota(jnp.int32, (rows, LANES), 1) < heads
        fixed[...] = jnp.zeros_like(fixed)
        for i, k in enumerate(early):
            at = lax.rem(where[0] + k, ring)
            below, above = (k - 1) % ring, (k + 1) % ring
            fade = fades[k][...]
            if below == late:
                fade = jnp.where(forward & (row < pad), 0.0, fade)
            if above == late:
                fade = jnp.where(jnp.logical_not(forward) & (row >= rows - pad), 0.0, fade)
            qs[i * rows : (i + 1) * rows, :] = two_parts(fade, 2 * heads)
            for n in range(0, channels, 256):
                cols = slice(n, n + 256)
                own = ends[k][: 2 * pad, cols].astype(F32)
                if below != late:
                    outer = ends[bounded][2 * pad : 3 * pad, cols]
                    before = jnp.where(at == 0, outer, ends[below][pad : 2 * pad, cols]).astype(F32)
                    window = jnp.concatenate([before, own[:pad]], axis=0)
                    fixed[k, :pad, cols] = conv_of(
                        window[pad - reach :], taps[0, :, cols], False, pad
                    ).astype(BF16)
                if above != late:
                    outer = ends[bounded][3 * pad :, cols]
                    after = jnp.where(at == ring - 1, outer, ends[above][:pad, cols]).astype(F32)
                    window = jnp.concatenate([own[pad:], after], axis=0)
                    fixed[k, pad:, cols] = conv_of(
                        window[: pad + reach], taps[1, :, cols], True, pad
                    ).astype(BF16)
        for d in range(2):
            for n in range(0, channels, 256):
                cols = slice(n, n + 256)
                scale = dot(qs[...], spread[d, :, cols])
                for i, k in enumerate(early):
                    x = patched((xf, xb)[d][k], fixed, k, cols, pad, d)
                    part = slice(i * rows, (i + 1) * rows)
                    added[i, d, :, cols] = dot(b_t[k][d], (scale[part] * x.astype(F32)).astype(BF16))

    return pl.pallas_call(
        body,
        in_specs=[smem()] + [vmem()] * (5 * count + 2),
        out_specs=[vmem()] * 2,
        out_shape=[
            jax.ShapeDtypeStruct((ring, 2 * pad, channels), BF16),
            jax.ShapeDtypeStruct((count, 2, size, channels), F32),
        ],
        scratch_shapes=[pltpu.VMEM((count * rows, LANES), BF16)],
        compiler_params=mib(16),
        cost_estimate=pl.CostEstimate(flops=1_000_000_000, bytes_accessed=4 << 20, transcendentals=0),
        name="early_sums",
    )(where, *[v for group in needed for v in group], taps, spread)


def combine(where, early, late, ring, blocks, bounded, lasts, fixed, added, taps, spread, heads):
    rows, channels = blocks[0][0].shape
    size = blocks[0][4].shape[1]
    pad = 8
    reach = taps.shape[1] - 1
    below, above = (late - 1) % ring, (late + 1) % ring
    sides = {k: i for i, k in enumerate(dict.fromkeys((late, below, above, bounded)))}
    count = len(sides)
    needed = [blocks[k][i] for i in (2, 4, 8) for k in sides]

    def body(where, *refs):
        ends, b_t, fades = (
            {k: refs[i * count + j] for k, j in sides.items()} for i in range(3)
        )
        refs = refs[3 * count :]
        xf, xb, early_fixed, added = refs[:4]
        lasts = refs[4 : 4 + ring]
        taps, spread, pack, fixed, carried = refs[4 + ring :]
        at, logs, between = frame_logs(where, lasts, ring)
        forward = lax.broadcasted_iota(jnp.int32, logs[0].shape, 1) < heads
        later = [jnp.where(forward, between(p, ring), between(-1, p)) for p in at]
        fixed[...] = early_fixed[...]

        def mend(k, d):
            first, final = at[k] == 0, at[k] == ring - 1
            for n in range(0, channels, 256):
                cols = slice(n, n + 256)
                own = ends[k][: 2 * pad, cols].astype(F32)
                if d == 0:
                    outer = ends[bounded][2 * pad : 3 * pad, cols]
                    next_to = ends[(k - 1) % ring][pad : 2 * pad, cols]
                    before = jnp.where(first, outer, next_to).astype(F32)
                    window = jnp.concatenate([before, own[:pad]], axis=0)[pad - reach :]
                    fixed[k, :pad, cols] = conv_of(window, taps[0, :, cols], False, pad).astype(BF16)
                else:
                    outer = ends[bounded][3 * pad :, cols]
                    next_to = ends[(k + 1) % ring][:pad, cols]
                    after = jnp.where(final, outer, next_to).astype(F32)
                    window = jnp.concatenate([own[pad:], after], axis=0)[: pad + reach]
                    fixed[k, pad:, cols] = conv_of(window, taps[1, :, cols], True, pad).astype(BF16)

        for k, d in ((late, 0), (late, 1), (above, 0), (below, 1)):
            mend(k, d)
        q = two_parts(fades[late][...] * jnp.exp2(later[late]), 2 * heads)
        q_above = two_parts(fades[above][:pad, :] * jnp.exp2(later[above]), 2 * heads)
        q_below = two_parts(fades[below][rows - pad :, :] * jnp.exp2(later[below]), 2 * heads)
        weights = spread_rows([later[k] for k in early], heads, spread)
        total = sum(logs[1:], logs[0])
        l1 = total.astype(BF16).astype(F32)
        l2 = (total - l1).astype(BF16).astype(F32)
        three = jnp.concatenate([l1, l2, total - l1 - l2, jnp.zeros((LOGS - 3, LANES), F32)], axis=0)
        carried[...] = jnp.zeros_like(carried)
        for d in range(2):
            pack[d, size:, :] = dot(three.astype(BF16), spread[d]).astype(BF16)
            side = above if d == 0 else below
            place = slice(rows, rows + pad) if d == 0 else slice(2 * rows - pad, 2 * rows)
            b_all = jnp.concatenate([b_t[late][d], b_t[side][d]], axis=1)
            for n in range(0, channels, 256):
                cols = slice(n, n + 256)
                x = patched((xf, xb)[d], fixed, late, cols, pad, d)
                scale = dot(q, spread[d, :, cols])
                carried[d, :rows, :] = (scale * x.astype(F32)).astype(BF16)
                scale = dot(q_above if d == 0 else q_below, spread[d, :, cols])
                x = fixed[side, :pad, cols] if d == 0 else fixed[side, pad:, cols]
                carried[d, place, :] = (scale * x.astype(F32)).astype(BF16)
                state = dot(b_all, carried[d])
                for i in range(len(early)):
                    state += weights[d][i : i + 1, cols] * added[i, d, :, cols]
                pack[d, :size, cols] = state.astype(BF16)

    return pl.pallas_call(
        body,
        in_specs=[smem()] + [vmem()] * (3 * count + 6 + ring),
        out_specs=[vmem()] * 2,
        out_shape=[
            jax.ShapeDtypeStruct((2, size + LOGS, channels), BF16),
            jax.ShapeDtypeStruct((ring, 2 * pad, channels), BF16),
        ],
        scratch_shapes=[pltpu.VMEM((2, 2 * rows, 256), BF16)],
        compiler_params=mib(16),
        cost_estimate=pl.CostEstimate(flops=500_000_000, bytes_accessed=4 << 20, transcendentals=0),
        name="combine",
    )(where, *needed, blocks[late][0], blocks[late][1], fixed, added, *lasts, taps, spread)


def patched(x, fixed, k, cols, pad, d):
    rows = x.shape[0]
    if d == 0:
        return jnp.concatenate([fixed[k, :pad, cols], x[pad:, cols]], axis=0)
    return jnp.concatenate([x[: rows - pad, cols], fixed[k, pad:, cols]], axis=0)


def starts_of(where, xfs, xbs, fixed, b_ts, fades, lasts, spread, heads):
    ring = len(xfs)
    rows, channels = xfs[0].shape
    size = b_ts[0].shape[1]
    pad = fixed.shape[1] // 2

    def body(where, *refs):
        xf, xb, b_t, fades, lasts = (refs[i * ring : (i + 1) * ring] for i in range(5))
        fixed, spread, starts, fades_out, qs = refs[5 * ring :]
        at, logs, between = frame_logs(where, lasts, ring)
        forward = lax.broadcasted_iota(jnp.int32, logs[0].shape, 1) < heads
        fade = spread_rows(
            [jnp.where(forward, between(-1, p), between(p, ring)) for p in at], heads, spread
        )
        for d in range(2):
            fades_out[d] = fade[d]
        for k in range(ring):
            qs[k * rows : (k + 1) * rows, :] = two_parts(fades[k][...], 2 * heads)
        weights = [
            spread_rows(
                [
                    jnp.where(forward, between(at[k], at[j]), between(at[j], at[k]))
                    for k in range(ring)
                ],
                heads,
                spread,
            )
            for j in range(ring)
        ]
        for d in range(2):
            for n in range(0, channels, 256):
                cols = slice(n, n + 256)
                scale = dot(qs[...], spread[d, :, cols])
                for k in range(ring):
                    x = patched((xf, xb)[d][k], fixed, k, cols, pad, d)
                    part = slice(k * rows, (k + 1) * rows)
                    added = dot(b_t[k][d], (scale[part] * x.astype(F32)).astype(BF16))
                    for j in range(ring):
                        if j == k:
                            continue
                        before = at[k] < at[j] if d == 0 else at[k] > at[j]
                        term = jnp.where(before, weights[j][d][k : k + 1, cols], 0.0) * added
                        if k == (1 if j == 0 else 0):
                            starts[j, d, :, cols] = term
                        else:
                            starts[j, d, :, cols] += term

    return pl.pallas_call(
        body,
        in_specs=[smem()] + [vmem()] * (5 * ring + 2),
        out_specs=[vmem()] * 2,
        out_shape=[
            jax.ShapeDtypeStruct((ring, 2, size, channels), F32),
            jax.ShapeDtypeStruct((2, ring + -ring % 8, channels), F32),
        ],
        scratch_shapes=[pltpu.VMEM((ring * rows, LANES), BF16)],
        compiler_params=mib(16),
        cost_estimate=pl.CostEstimate(flops=1_200_000_000, bytes_accessed=8 << 20, transcendentals=0),
        name="starts",
    )(where, *xfs, *xbs, *b_ts, *fades, *lasts, fixed, spread)


def inside(k, xf, xb, fixed, bc, cum, cum_t, skip, heads):
    rows, channels = xf.shape
    size = bc.shape[1] // 4

    pad = fixed.shape[1] // 2

    def body(xf, xb, fixed, bc, cum, cum_t, skip, y):
        row, col = (lax.broadcasted_iota(jnp.int32, (rows, rows), d) for d in (0, 1))
        first = lax.broadcasted_iota(jnp.int32, (rows, LANES), 1) < HEAD_DIM
        scores = []
        for d in range(2):
            b_rows = bc[:, 2 * d * size : (2 * d + 1) * size]
            c_rows = bc[:, (2 * d + 1) * size : (2 * d + 2) * size]
            s = lax.dot_general(
                c_rows, b_rows, (((1,), (1,)), ((), ())), preferred_element_type=F32
            )
            scores.append(jnp.where(row >= col if d == 0 else row <= col, s, 0.0))
        for pair in range(channels // LANES):
            cols = slice(pair * LANES, (pair + 1) * LANES)
            weights = []
            for h in range(pair * (LANES // HEAD_DIM), (pair + 1) * (LANES // HEAD_DIM)):
                sides = []
                for d in range(2):
                    at = d * heads + h
                    gap = jnp.minimum(cum[:, at : at + 1] - cum_t[at : at + 1, :], 0.0)
                    dt = cum_t[2 * heads + at : 2 * heads + at + 1, :]
                    sides.append((jnp.exp2(gap) * (scores[d] * dt)).astype(BF16))
                weights.append(jnp.concatenate(sides, axis=1))
            sides = [patched(x, fixed, k, cols, pad, d) for d, x in enumerate((xf, xb))]
            x_pair = jnp.concatenate(sides, axis=0)
            out = dot(jnp.concatenate(weights, axis=0), x_pair)
            total = jnp.where(first, out[:rows], out[rows:])
            total += skip[0:1, cols] * sides[0].astype(F32)
            total += skip[1:2, cols] * sides[1].astype(F32)
            y[:, cols] = total

    return pl.pallas_call(
        body,
        in_specs=[vmem()] * 7,
        out_specs=vmem(),
        out_shape=jax.ShapeDtypeStruct((rows, channels), F32),
        compiler_params=mib(12),
        cost_estimate=pl.CostEstimate(flops=1_200_000_000, bytes_accessed=2 << 20, transcendentals=0),
        name="inside",
    )(xf, xb, fixed, bc, cum, cum_t, skip)


def gates(pieces, w_gate, bc=None, w_state=None):
    rows, depth = sum(p.shape[0] for p in pieces), pieces[0].shape[1]
    channels, count = w_gate.shape[1], len(pieces)
    more = [] if bc is None else [bc, w_state]
    size = 0 if bc is None else bc.shape[1] // 4

    def body(*refs):
        wg, refs_ = refs[count], refs[count + 1 + len(more) :]
        gate, block = refs_[0], refs_[-1]
        gather(refs[:count], block)
        if more:
            old, ws, new = refs[count + 1], refs[count + 2], refs_[1]
            for d in range(2):
                b_cols = slice(2 * d * size, (2 * d + 1) * size)
                c_cols = slice((2 * d + 1) * size, (2 * d + 2) * size)
                new[:, b_cols] = old[:, b_cols]
                new[:, c_cols] = dot(block[...], ws[:, c_cols]).astype(BF16)
        for n in range(0, channels, 256):
            raw = dot(block[...], wg[:, n : n + 256]).astype(BF16)
            gate[:, n : n + 256] = silu(raw.astype(F32))

    shapes = [jax.ShapeDtypeStruct((rows, channels), F32)]
    if more:
        shapes.append(jax.ShapeDtypeStruct(bc.shape, BF16))
    return pl.pallas_call(
        body,
        in_specs=[vmem()] * (count + 1 + len(more)),
        out_specs=[vmem()] * len(shapes),
        out_shape=shapes,
        scratch_shapes=[pltpu.VMEM((rows, depth), BF16)],
        compiler_params=mib(12),
        cost_estimate=pl.CostEstimate(
            flops=2 * rows * depth * channels, bytes_accessed=2 * depth * channels, transcendentals=0
        ),
        name="gates",
    )(*pieces, w_gate, *more)


def log_rows(rows):
    rows = rows.astype(F32)
    return rows[0:1] + rows[1:2] + rows[2:3]


def messages(where, mine, theirs, groups, parts):
    size, channels = mine.shape[1] - LOGS, mine.shape[2]
    width = channels // parts

    def body(where, mine, theirs, *outs):
        group, second = where[1], where[2] == 1
        cols = pl.ds(pl.multiple_of(where[2] * width, LANES), width)
        for d in range(2):
            own, other = log_rows(mine[d, size:, cols]), log_rows(theirs[d, size:, cols])
            later = second if d == 0 else jnp.logical_not(second)
            scale_own = jnp.where(later, 1.0, jnp.exp2(other))
            scale_other = jnp.where(later, jnp.exp2(own), 1.0)
            total = own + other
            l1 = total.astype(BF16).astype(F32)
            l2 = (total - l1).astype(BF16).astype(F32)
            logs = jnp.concatenate(
                [l1, l2, total - l1 - l2, jnp.zeros((LOGS - 3, width), F32)], axis=0
            ).astype(BF16)
            state = scale_own * mine[d, :size, cols].astype(F32)
            state = (state + scale_other * theirs[d, :size, cols].astype(F32)).astype(BF16)
            for k, out in enumerate(outs, 1):
                onward = group + k < groups

                @pl.when(onward if d == 0 else jnp.logical_not(onward))
                def _(out=out):
                    out[:size, :] = state
                    out[size:, :] = logs

    return pl.pallas_call(
        body,
        in_specs=[smem(), vmem(), vmem()],
        out_specs=[vmem()] * (groups - 1),
        out_shape=[jax.ShapeDtypeStruct((size + LOGS, width), BF16)] * (groups - 1),
        compiler_params=mib(16),
        cost_estimate=pl.CostEstimate(flops=1_000_000, bytes_accessed=2 << 20, transcendentals=0),
        name="messages",
    )(where, mine, theirs)


def entering(where, received, groups):
    size, width = received[0].shape[0] - LOGS, received[0].shape[1]

    def body(where, *refs):
        got, out = refs[:-1], refs[-1]
        group = where[1]
        for d in range(2):
            log = jnp.zeros((1, width), F32)
            state = jnp.zeros((size, width), F32)
            for far in range(1, groups):
                ref = got[far - 1] if d == 0 else got[groups - far - 1]
                holds = far <= (group if d == 0 else groups - 1 - group)
                scale = jnp.where(holds, jnp.exp2(log), 0.0)
                state += scale * ref[:size, :].astype(F32)
                log = jnp.where(holds, log + log_rows(ref[size:, :]), log)
            out[d] = state.astype(BF16)

    return pl.pallas_call(
        body,
        in_specs=[smem()] + [vmem()] * len(received),
        out_specs=vmem(),
        out_shape=jax.ShapeDtypeStruct((2, size, width), BF16),
        compiler_params=mib(16),
        cost_estimate=pl.CostEstimate(flops=1_000_000, bytes_accessed=2 << 20, transcendentals=0),
        name="entering",
    )(where, *received)


SUB = 16


def pack_squares(row):
    high = row.astype(BF16).astype(F32)
    return jnp.concatenate([high, row - high, jnp.zeros((SUB - 2, LANES), F32)], axis=0).astype(BF16)


def squares_of(packed):
    v = packed.astype(F32)
    return v[0:1] + v[1:2]


def finish(where, k, y, bc, reached, gate, starts, fades, theirs, mine, other, spread, gain, w_out):
    rows, channels = y.shape
    size = bc.shape[1] // 4
    width = w_out.shape[1]
    half = rows // 2
    last = k == 0
    part = mine.shape[2]
    step = min(256, part)
    across = width // LANES
    count = half // SUB * across

    def body(where, y, bc, reached, gate, starts, fades, theirs, mine, other, spread, gain, w_out, *refs):
        outs, scaled = refs[:-1], refs[-1]
        second = where[2] == 1
        square = jnp.zeros((rows, LANES), F32)
        for n in range(0, channels, step):
            cols = slice(n, n + step)
            total = y[:, cols]
            for d in range(2):
                c_rows = bc[:, (2 * d + 1) * size : (2 * d + 2) * size]
                near = second if d == 0 else jnp.logical_not(second)
                at = slice(n % part, n % part + step)
                enter = jnp.where(where[2] == n // part, mine[d, :, at], other[d, :, at]).astype(F32)
                log = jnp.where(near, log_rows(theirs[d, size:, cols]), 0.0)
                enter = jnp.exp2(log) * enter
                enter += jnp.where(near, theirs[d, :size, cols].astype(F32), 0.0)
                state = starts[0, d, :, cols] + fades[d, k : k + 1, cols] * enter
                total += dot(reached[...], spread[d, :, cols]) * dot(c_rows, state.astype(BF16))
            gated = total * gate[:, cols]
            for t in range(0, step, LANES):
                square += gated[:, t : t + LANES] * gated[:, t : t + LANES]
            scaled[:, cols] = (gated * gain[:, cols]).astype(BF16)
        sums = jnp.broadcast_to(jnp.sum(square, axis=1, keepdims=True), (rows, LANES))
        row = sums.T[0:1, :]
        if last:
            outs[1][...] = jnp.broadcast_to(row, (SUB, rows))
        else:
            for out in outs:
                out[count] = pack_squares(row)
        for n in range(0, width, 256):
            value = dot(scaled[...], w_out[:, n : n + 256])
            if last:
                outs[0][:, n : n + 256] = value
                continue
            value = value.astype(BF16)
            for i in range(rows // SUB):
                for j in range(0, 256, LANES):
                    tile = value[i * SUB : (i + 1) * SUB, j : j + LANES]
                    place = i % (half // SUB) * across + (n + j) // LANES
                    outs[i * SUB // half][place] = tile

    if last:
        shapes = [((rows, width), F32), ((SUB, rows), F32)]
    else:
        shapes = [((count + 1, SUB, LANES), BF16)] * 2
    specs = [smem()] + [vmem()] * 12
    specs[5] = pl.BlockSpec((1,) + starts.shape[1:], lambda i: (k, 0, 0, 0))
    return pl.pallas_call(
        body,
        grid=(1,),
        in_specs=specs,
        out_specs=[vmem()] * len(shapes),
        out_shape=[jax.ShapeDtypeStruct(*s) for s in shapes],
        scratch_shapes=[pltpu.VMEM((rows, channels), BF16)],
        compiler_params=mib(16),
        cost_estimate=pl.CostEstimate(
            flops=2 * rows * channels * width, bytes_accessed=2 * channels * width, transcendentals=0
        ),
        name="finish",
    )(where, y, bc, reached, gate, starts, fades, theirs, mine, other, spread, gain, w_out)


def plus(value, got):
    count = value.shape[0] - 1

    def body(value, got, out):
        for n in range(0, count, 8):
            part = slice(n, min(n + 8, count))
            out[part] = (value[part].astype(F32) + got[part].astype(F32)).astype(BF16)
        out[count] = pack_squares(squares_of(value[count]) + squares_of(got[count]))

    return pl.pallas_call(
        body,
        in_specs=[vmem()] * 2,
        out_specs=vmem(),
        out_shape=jax.ShapeDtypeStruct(value.shape, BF16),
        compiler_params=mib(8),
        name="plus",
    )(value, got)


def normalize(part, into, value, square, got, channels):
    rows, width = value.shape
    half = rows // 2
    across = width // LANES
    count = half // SUB * across
    held = [] if into is None else [into]

    def body(value, square, *refs):
        ins, out = refs[: len(got)], refs[-1]
        sums = square[0:1, :]
        for ref in ins:
            sums = sums + squares_of(ref[count])
        scale = lax.rsqrt(sums / channels + 1e-05)
        scale = jnp.broadcast_to(scale, (LANES, rows)).T[part * half : (part + 1) * half]
        for i in range(half // SUB):
            for j in range(across):
                at = (slice(i * SUB, (i + 1) * SUB), slice(j * LANES, (j + 1) * LANES))
                total = value[at]
                for ref in ins:
                    total = total + ref[i * across + j].astype(F32)
                out[at] = (total * scale[at[0], :]).astype(BF16)

    block = pl.BlockSpec((half, width), lambda n: (part, 0))
    return pl.pallas_call(
        body,
        grid=(1,),
        in_specs=[block] + [vmem()] * (1 + len(got)) + [pl.BlockSpec(memory_space=pl.ANY)] * len(held),
        out_specs=block,
        out_shape=jax.ShapeDtypeStruct(value.shape, BF16),
        input_output_aliases={2 + len(got): 0} if held else {},
        compiler_params=mib(8),
        name="normalize",
    )(value, square, *got, *held)


def ring_pairs(count, step):
    return [(i, (i + step) % count) for i in range(count)]


def layer(
    tokens,
    w_gate,
    w_value,
    w_state_proj,
    w_step,
    step_bias,
    decay_rate,
    conv_taps,
    skip_gain,
    norm_gain,
    w_out,
):
    ring, frames = lax.axis_size("row"), lax.axis_size("frame")
    row, frame = lax.axis_index("row"), lax.axis_index("frame")
    channels, heads = w_gate.shape[1], step_bias.shape[1]
    span = 2 if frames % 2 == 0 else 1
    groups = frames // span
    where = jnp.stack([row, frame // span, frame % span]).astype(jnp.int32)
    own = tokens.reshape(-1, tokens.shape[2])
    far = ring // 2
    edge = 8
    end = ring - 1

    def up(v):
        return lax.ppermute(v, "row", ring_pairs(ring, 1))

    def down(v):
        return lax.ppermute(v, "row", ring_pairs(ring, -1))

    first, second, outer = split(where, own, ring, edge)
    pieces = {0: [first, second]}
    order = [0]
    from_below, from_above = [first, second], [second, first]
    for hop in range(1, far + 1):
        a, c = up(from_below[0]), down(from_above[0])
        if 2 * hop == ring:
            pieces[hop] = [a, c]
            order.append(hop)
        else:
            b, d = up(from_below[1]), down(from_above[1])
            from_below, from_above = [a, b], [c, d]
            pieces[ring - hop], pieces[hop] = [a, b], [d, c]
            order += [ring - hop, hop]
    bounds = []
    for j in range(ring):
        pairs = [(f * ring + end, (f + 1) * ring + (end + j) % ring) for f in range(frames - 1)]
        pairs += [((f + 1) * ring, f * ring + j) for f in range(frames - 1)]
        bounds.append(lax.ppermute(outer, ("frame", "row"), pairs))

    steps = jnp.swapaxes(w_step, 1, 2).reshape(-1, w_step.shape[1])
    spread, small_rows, skip = prepare(step_bias, decay_rate, skip_gain, channels)
    gain = norm_gain.reshape(1, -1)

    blocks = {}
    bounded = order[-2]
    for k in order:
        blocks[k] = block_states(
            pieces[k],
            bounds if k == bounded else [],
            where,
            w_value,
            w_state_proj,
            steps,
            conv_taps,
            small_rows,
            heads,
            k == order[-1],
        )
    xfs, xbs, _, bcs, b_ts, cums, cum_ts, reached, fading, lasts = (
        [blocks[k][i] for k in range(ring)] for i in range(len(blocks[0]))
    )
    early, late = order[:-1], order[-1]
    shared = (early, late, ring, blocks, bounded)
    fixed, added = early_sums(where, *shared, conv_taps, spread, heads)
    pack, fixed = combine(where, *shared, lasts, fixed, added, conv_taps, spread, heads)

    if span == 2:
        swap = [(i, i ^ 1) for i in range(frames)]
        theirs = lax.ppermute(pack, "frame", swap)
    else:
        theirs = jnp.zeros_like(pack)
    received = []
    if groups > 1:
        sends = messages(where, pack, theirs, groups, span)
        for k in sorted(range(1, groups), key=lambda k: k % 2 == 0):
            pairs = [
                (g * span + s, (g + k) % groups * span + s) for g in range(groups) for s in range(span)
            ]
            received.append((k, lax.ppermute(sends[k - 1], "frame", pairs)))
        received = [v for _, v in sorted(received, key=lambda kv: kv[0])]
        enter = entering(where, received, groups)
    else:
        enter = jnp.zeros((2, pack.shape[1] - LOGS, channels // span), BF16)
    other = lax.ppermute(enter, "frame", swap) if span == 2 else enter
    inner, gate = {}, {}
    for k in order:
        if k == late:
            gate[k], bcs[k] = gates(pieces[k], w_gate, bcs[k], w_state_proj)
        else:
            (gate[k],) = gates(pieces[k], w_gate)
        inner[k] = inside(k, xfs[k], xbs[k], fixed, bcs[k], cums[k], cum_ts[k], skip, heads)
    starts, fades = starts_of(where, xfs, xbs, fixed, b_ts, fading, lasts, spread, heads)

    def block(k):
        return finish(
            where,
            k,
            inner[k],
            bcs[k],
            reached[k],
            gate[k],
            starts,
            fades,
            theirs,
            enter,
            other,
            spread,
            gain,
            w_out,
        )

    up_a = up_b = down_a = down_b = None
    for hop in range(far, 0, -1):
        if 2 * hop == ring:
            a, b = block(hop)
            up_a, down_b = up(a), down(b)
            continue
        (above_a, above_b), (below_a, below_b) = block(hop), block(ring - hop)
        up_b = up(above_b if up_b is None else plus(above_b, up_b))
        down_a = down(below_a if down_a is None else plus(below_a, down_a))
        up_a = up(above_a if up_a is None else plus(above_a, up_a))
        down_b = down(below_b if down_b is None else plus(below_b, down_b))
    value, square = block(0)
    halves = [[v for v in pair if v is not None] for pair in ((up_a, down_a), (up_b, down_b))]
    mixed = normalize(FIRST, None, value, square, halves[FIRST], channels * ring)
    mixed = normalize(1 - FIRST, mixed, value, square, halves[1 - FIRST], channels * ring)
    return mixed.reshape(tokens.shape)


def solution(mesh):
    return jax.shard_map(
        layer,
        mesh=mesh,
        in_specs=(
            P("frame", "row", None),
            P(None, "row"),
            P(None, "row"),
            P(),
            P(None, None, "row"),
            P(None, "row"),
            P(None, "row"),
            P(None, None, "row"),
            P(None, "row"),
            P("row"),
            P("row", None),
        ),
        out_specs=P("frame", "row", None),
        check_vma=False,
    )
```
